32 devices in a mesh: row: 4 (over y, core), col: 8 (over z, x).
Axes of the slice: x: 2, y: 2, z: 4, core: 2. Of those that a mesh axis runs over, the one named last changes fastest.
Arguments:
- right_side: float32 [5, 2, 64, 2048], P(None, None, None, 'row'), may hold values from -6 to 6
- panels: float32 [10, 2, 2048, 2048], P(None, None, 'row', 'col'), may hold values from -0.0625 to 0.0625
- diag_inverse: float32 [5, 2, 2048, 2048], P(None, None, 'row', 'col'), may hold values from -0.026516504 to 1.4
- parents: int32 [4, 2], replicated, may hold values from 0 to 1
- live_width: int32 [5, 2], replicated, may hold values from 1024 to 2048
- tile_pattern: int32 [10, 2, 16], replicated, may hold values 0 or 1
Outputs:
- interim: float32 [5, 2, 64, 2048], P(None, None, None, 'row')
- solution: float32 [5, 2, 64, 2048], P(None, None, None, 'row')
The draws below stay inside these ranges and needn't reach their ends.
Inputs may be any that keep to these rules, and one draw needn't show every extreme that they name: parents[h, k] is the position on level h + 1 of the parent of supernode (h, k). The columns of supernode (h, k) from live_width[h, k] up to 2048 are padding. `tile_pattern`: 1 where the tile of 128 rows is present in the block.
All inputs are finite; a program needn't handle non-finite values.
Results may differ from the reference program's by a relative error of at most 0.0001.
Values sent between devices are 32-bit elements; how exact they have to be, the bound alone decides.
No kernel may reach another device: no remote copies, remote signals or barrier semaphores. Data moves between devices by JAX's collectives and lax.ppermute only.
A program may use at most 64 MiB of HBM per device.

```python
import jax
import jax.numpy as jnp
from jax import lax

SNW = 2048
NRHS = 64
TILE = 128
STEPS = 5
PER = 2
PAIRS = 10


def draw_diag_inverse(key, part):
    diag_key, noise_key = jax.random.split(jax.random.fold_in(key, 11))
    spread = 0.4 * SNW ** (-0.5)
    diagonal = jax.random.uniform(diag_key, (STEPS, PER, SNW), jnp.float32, 0.6, 1.4)
    off_diag = spread * jax.random.truncated_normal(noise_key, -3.0, 3.0, (STEPS, PER, SNW, SNW), jnp.float32)
    eye_mask = jnp.eye(SNW, dtype=jnp.float32)
    return off_diag * (1.0 - eye_mask) + diagonal[:, :, :, None] * eye_mask


def place_ends(drawn, rng, least, top_value):
    index_at = [jax.random.randint(jax.random.fold_in(rng, axis), (), 0, length) for axis, length in enumerate(drawn.shape)]
    main_axis = drawn.shape.index(max(drawn.shape))
    beside = index_at[:main_axis] + [(index_at[main_axis] + 1) % drawn.shape[main_axis]] + index_at[main_axis + 1:]
    return drawn.at[tuple(index_at)].set(least).at[tuple(beside)].set(top_value)


def level_of(own_key, dims, pieces, smallest, largest):
    level = 1.0
    for axis_at, blocks in pieces:
        draws = jax.random.uniform(jax.random.fold_in(jax.random.fold_in(own_key, 6), axis_at), (blocks,), jnp.float32, smallest / len(pieces), largest / len(pieces))
        level = level * jnp.repeat(jnp.exp(draws), dims[axis_at] // blocks).reshape((-1,) + (1,) * (len(dims) - 1 - axis_at))
    return level


def gaussian(stream_key, shape, deviation, limit, shards=(), held_as=jnp.bfloat16):
    array = jax.random.normal(stream_key, shape, jnp.float32) * deviation
    if len(shards) > 0:
        array = level_of(stream_key, shape, shards, -0.22, 0.18) * array
    return jnp.clip(array, min=-limit, max=limit).astype(held_as)


def setup_inputs(seed: int = 0) -> dict:
    seeds = jax.random.split(jax.random.key(seed), 7)
    right_side = gaussian(seeds[0], (STEPS, PER, NRHS, SNW), 1.0, 6.0, ((3, 4),), jnp.float32)
    panels = gaussian(seeds[1], (PAIRS, PER, SNW, SNW), (4 * SNW) ** -0.5, 0.0625, ((2, 4), (3, 8)), jnp.float32)
    diag_inverse = draw_diag_inverse(jax.random.fold_in(seeds[6], 71), 0)
    parents = place_ends(jax.random.randint(seeds[3], (STEPS - 1, PER), 0, PER), jax.random.fold_in(seeds[3], 1), 0, PER - 1).astype(jnp.int32)
    live_width = place_ends(jax.random.randint(seeds[4], (STEPS, PER), SNW // 2, SNW + 1), jax.random.fold_in(seeds[4], 1), SNW // 2, SNW).astype(jnp.int32)
    tile_pattern = place_ends((jax.random.randint(seeds[5], (PAIRS, PER, SNW // TILE), 0, 4) < 3).astype(jnp.int32), jax.random.fold_in(seeds[5], 1), 0, 1)
    return {"right_side": right_side, "panels": panels, "diag_inverse": diag_inverse, "parents": parents, "live_width": live_width, "tile_pattern": tile_pattern}


HIGHEST_PRECISION = lax.Precision.HIGHEST


def pair_index(lower, higher, depth_count):
    return lower * depth_count - lower * (lower + 1) // 2 + (higher - lower - 1)


def climb_maps(parents):
    depth_count = parents.shape[0] + 1
    width_count = parents.shape[1]
    positions = jnp.arange(width_count, dtype=jnp.int32)
    hop_maps = [(parents[height][:, None] == positions[None, :]).astype(jnp.float32) for height in range(depth_count - 1)]
    climbs = {}
    for height in range(depth_count - 1):
        current = hop_maps[height]
        climbs[(height, height + 1)] = current
        for higher in range(height + 2, depth_count):
            current = jnp.dot(current, hop_maps[higher - 1], precision=HIGHEST_PRECISION)
            climbs[(height, higher)] = current
    return climbs


def reference(right_side, panels, diag_inverse, parents, live_width, tile_pattern):
    levels = STEPS
    width_mask = (jnp.arange(SNW, dtype=jnp.int32)[None, None, :] < live_width[:, :, None]).astype(jnp.float32)
    rows_mask = jnp.repeat(tile_pattern.astype(jnp.float32), TILE, axis=2)
    climbs = climb_maps(parents)
    pending = [jnp.zeros((PER, NRHS, SNW), jnp.float32) for height in range(levels)]
    interim = []
    for height in range(levels):
        residual = (right_side[height] - pending[height]) * width_mask[height][:, None, :]
        solved = jnp.einsum("kab,kjb->kja", diag_inverse[height], residual, precision=HIGHEST_PRECISION)
        solved = solved * width_mask[height][:, None, :]
        interim.append(solved)
        for higher in range(height + 1, levels):
            block_slot = pair_index(height, higher, levels)
            update_term = jnp.einsum("kab,kjb->kja", panels[block_slot], solved, precision=HIGHEST_PRECISION)
            update_term = update_term * rows_mask[block_slot][:, None, :]
            pending[higher] = pending[higher] + jnp.einsum("kt,kja->tja", climbs[(height, higher)], update_term, precision=HIGHEST_PRECISION)
    solution = [None] * levels
    for height in reversed(range(levels)):
        carried = jnp.zeros((PER, NRHS, SNW), jnp.float32)
        for higher in range(height + 1, levels):
            block_slot = pair_index(height, higher, levels)
            ancestor_part = jnp.einsum("kt,tja->kja", climbs[(height, higher)], solution[higher], precision=HIGHEST_PRECISION)
            ancestor_part = ancestor_part * rows_mask[block_slot][:, None, :]
            carried = carried + jnp.einsum("kab,kja->kjb", panels[block_slot], ancestor_part, precision=HIGHEST_PRECISION)
        residual = (interim[height] - carried) * width_mask[height][:, None, :]
        solved_back = jnp.einsum("kab,kja->kjb", diag_inverse[height], residual, precision=HIGHEST_PRECISION)
        solution[height] = solved_back * width_mask[height][:, None, :]
    return jnp.stack(interim), jnp.stack(solution)
```

```python
import jax
import jax.numpy as jnp
from jax import lax
from jax.sharding import PartitionSpec as P

TILE = 128
PRECISION = lax.Precision.HIGH


def pair_index(lower, higher, depth_count):
    return lower * depth_count - lower * (lower + 1) // 2 + (higher - lower - 1)


def climb_maps(parents):
    depth_count, width_count = parents.shape[0] + 1, parents.shape[1]
    positions = jnp.arange(width_count, dtype=jnp.int32)
    climbs = {}
    for height in range(depth_count - 1):
        place = parents[height]
        climbs[height, height + 1] = (place[:, None] == positions).astype(jnp.float32)
        for higher in range(height + 2, depth_count):
            step = parents[higher - 1]
            place = sum(jnp.where(place == k, step[k], 0) for k in range(width_count))
            climbs[height, higher] = (place[:, None] == positions).astype(jnp.float32)
    return climbs


def solution(mesh):
    row_count, col_count = mesh.shape["row"], mesh.shape["col"]
    y_count = row_count // 2
    groups = col_count // y_count
    assert row_count == 2 * y_count and col_count == groups * y_count
    assert groups >= 2 and groups & (groups - 1) == 0
    axes = ("row", "col")

    def pairs(move):
        found = []
        for row in range(row_count):
            for col in range(col_count):
                y, core, q, g = move(row // 2, row % 2, col // groups, col % groups)
                found.append((row * col_count + col, (2 * y + core) * col_count + groups * q + g))
        return found

    swap_pairs = pairs(lambda y, core, q, g: (y, 1 - core, q, g))
    group_pairs = [pairs(lambda y, core, q, g, k=k: (y, core, q, g ^ k)) for k in range(groups)]
    turn_pairs = [
        pairs(lambda y, core, q, g, t=t: ((q + t) % y_count, core, y, g)) for t in range(y_count)
    ]
    back_pairs = [[(b, a) for a, b in some] for some in turn_pairs]

    def move(values, some):
        return lax.ppermute(values, axes, some)

    def per_device(right_side, panels, diag_inverse, parents, live_width, tile_pattern):
        levels, per_level, rhs_count, row_span = right_side.shape
        col_span = panels.shape[3]
        half = rhs_count // 2
        row, col = lax.axis_index("row"), lax.axis_index("col")
        core, y = row % 2, row // 2
        g = col % groups
        top = groups // 2
        flip = (core != g // top)

        def live(first, span):
            cells = first + jnp.arange(span, dtype=jnp.int32)
            return (cells < live_width[:, :, None]).astype(jnp.float32)[:, :, None, :]

        col_live = live(col * col_span, col_span)
        own_live = live(row * row_span, row_span)
        mate = row + 1 - 2 * core
        mate_live = live(mate * row_span, row_span)
        tile_count = row_span // TILE

        def keep(place):
            tiles = lax.dynamic_slice_in_dim(tile_pattern, place * tile_count, tile_count, 2)
            return jnp.repeat(tiles.astype(jnp.float32), TILE, axis=2)[:, :, None, :]

        own_keep, mate_keep = keep(row), keep(mate)
        climbs = climb_maps(parents)

        def to_pieces(own, mates):
            first, second = jnp.where(flip, mates, own), jnp.where(flip, own, mates)
            pieces = []
            for part in (first, second):
                pieces += [part[..., i * col_span : (i + 1) * col_span] for i in range(top)]
            bit = 1
            while bit < top:
                on = (g & bit) != 0
                pieces = [jnp.where(on, pieces[k ^ bit], pieces[k]) for k in range(groups)]
                bit *= 2
            return pieces

        def from_pieces(pieces):
            bit = 1
            while bit < top:
                on = (g & bit) != 0
                pieces = [jnp.where(on, pieces[k ^ bit], pieces[k]) for k in range(groups)]
                bit *= 2
            first = jnp.concatenate(pieces[:top], axis=-1)
            second = jnp.concatenate(pieces[top:], axis=-1)
            return jnp.where(flip, second, first), jnp.where(flip, first, second)

        def rows_to_cols(own, mates):
            pieces = to_pieces(own, mates)
            moved = [move(pieces[k], group_pairs[k]) for k in range(1, groups)]
            summed = sum(moved, pieces[0])
            turned = [move(summed, some) for some in turn_pairs]
            return sum(turned[1:], turned[0])

        def spread(block):
            return from_pieces([block] + [move(block, group_pairs[k]) for k in range(1, groups)])

        def cols_to_rows(values):
            turned = [move(values, some) for some in back_pairs]
            return spread(sum(turned[1:], turned[0]))

        def halves(values, which):
            return lax.dynamic_slice_in_dim(values, which * half, half, 2)

        def whole(own, mates):
            theirs = move(mates, swap_pairs)
            first, second = jnp.where(core == 0, own, theirs), jnp.where(core == 0, theirs, own)
            return jnp.concatenate([first, second], axis=2)

        def down(block, values):
            return jnp.einsum("kab,kjb->kja", block, values, precision=PRECISION)

        def up(block, values):
            return jnp.einsum("kab,kja->kjb", block, values, precision=PRECISION)

        own_side = halves(right_side, core)
        mate_side = move(halves(right_side, 1 - core), swap_pairs)
        mate_diag = move(diag_inverse, swap_pairs)
        mate_panels = move(panels, swap_pairs)

        once = (col == 0).astype(jnp.float32)
        own_rest = [own_side[h] * once for h in range(levels)]
        mate_rest = [mate_side[h] * once for h in range(levels)]
        interim = []
        for height in range(levels):
            if height == 0:
                residual = move(to_pieces(own_side[0], mate_side[0])[0], turn_pairs[0])
            else:
                residual = rows_to_cols(own_rest[height], mate_rest[height])
            residual = residual * col_live[height]
            solved = rows_to_cols(
                down(diag_inverse[height], residual), down(mate_diag[height], residual)
            )
            solved = solved * col_live[height]
            interim.append(solved)
            for higher in range(height + 1, levels):
                slot = pair_index(height, higher, levels)
                climb = climbs[height, higher][:, :, None, None]

                def update(block, kept):
                    term = down(block, solved) * kept
                    return jnp.sum(climb * term[:, None], axis=0)

                own_rest[higher] = own_rest[higher] - update(panels[slot], own_keep[slot])
                mate_rest[higher] = mate_rest[higher] - update(mate_panels[slot], mate_keep[slot])

        interim_own, interim_mate = spread(move(jnp.stack(interim), back_pairs[0]))
        interim_rows = whole(interim_own, interim_mate)

        first_y = (y == 0).astype(jnp.float32)
        found = [None] * levels
        for height in reversed(range(levels)):
            if height + 1 < levels:
                rest = interim[height] * first_y
                for higher in range(height + 1, levels):
                    slot = pair_index(height, higher, levels)
                    climb = climbs[height, higher][:, :, None, None]

                    def carried(block, kept, values):
                        part = jnp.sum(climb * values[None], axis=1) * kept
                        return up(block, part)

                    rest = rest - carried(panels[slot], own_keep[slot], found[higher][0])
                    rest = rest - carried(mate_panels[slot], mate_keep[slot], found[higher][1])
                own, mates = cols_to_rows(rest)
            else:
                own, mates = interim_own[height], interim_mate[height]
            back = up(diag_inverse[height], own * own_live[height])
            back = back + up(mate_diag[height], mates * mate_live[height])
            found[height] = cols_to_rows(back * col_live[height])
        found_own = jnp.stack([pair[0] for pair in found])
        found_mate = jnp.stack([pair[1] for pair in found])
        return interim_rows, whole(found_own, found_mate)

    return jax.shard_map(
        per_device,
        mesh=mesh,
        in_specs=(
            P(None, None, None, "row"),
            P(None, None, "row", "col"),
            P(None, None, "row", "col"),
            P(),
            P(),
            P(),
        ),
        out_specs=(P(None, None, None, "row"), P(None, None, None, "row")),
        check_vma=False,
    )
```

```python
import jax
import jax.numpy as jnp
from jax import lax
from jax.experimental import pallas as pl
from jax.experimental.pallas import tpu as pltpu
from jax.sharding import PartitionSpec as P

TILE = 128


VMEM = pl.BlockSpec(memory_space=pltpu.VMEM)


def pair_index(lower, higher, depth_count):
    return lower * depth_count - lower * (lower + 1) // 2 + (higher - lower - 1)


def climb_maps(parents):
    depth_count, width_count = parents.shape[0] + 1, parents.shape[1]
    positions = jnp.arange(width_count, dtype=jnp.int32)
    climbs = {}
    for height in range(depth_count - 1):
        place = parents[height]
        climbs[height, height + 1] = (place[:, None] == positions).astype(jnp.float32)
        for higher in range(height + 2, depth_count):
            step = parents[higher - 1]
            place = sum(jnp.where(place == k, step[k], 0) for k in range(width_count))
            climbs[height, higher] = (place[:, None] == positions).astype(jnp.float32)
    return climbs


def limbs_of(values, count):
    parts = []
    rest = values
    for i in range(count):
        part = rest.astype(jnp.bfloat16)
        parts.append(part)
        if i + 1 < count:
            rest = rest - part.astype(jnp.float32)
    return parts


def product(values, large, small, contract_block):
    m = values.shape[0]
    left = limbs_of(values, 3)
    total = None
    for block, count in ((small, 2), (large, 3)):
        found = lax.dot_general(
            jnp.concatenate(left[:count], axis=0),
            block,
            (((1,), (contract_block,)), ((), ())),
            preferred_element_type=jnp.float32,
        )
        for n in reversed(range(count)):
            part = found[n * m : (n + 1) * m]
            total = part if total is None else total + part
    return total


def solution(mesh):
    row_count, col_count = mesh.shape["row"], mesh.shape["col"]
    y_count = row_count // 2
    groups = col_count // y_count
    assert row_count == 2 * y_count and col_count == groups * y_count
    assert groups >= 2 and groups & (groups - 1) == 0
    top = groups // 2
    axes = ("row", "col")

    def pairs(move):
        found = []
        for row in range(row_count):
            for col in range(col_count):
                y, core, q, g = move(row // 2, row % 2, col // groups, col % groups)
                found.append((row * col_count + col, (2 * y + core) * col_count + groups * q + g))
        return found

    swap_pairs = pairs(lambda y, core, q, g: (y, 1 - core, q, g))
    group_pairs = [pairs(lambda y, core, q, g, k=k: (y, core, q, g ^ k)) for k in range(groups)]
    turn_pairs = [
        pairs(lambda y, core, q, g, t=t: ((q + t) % y_count, core, y, g)) for t in range(y_count)
    ]
    back_pairs = [[(b, a) for a, b in some] for some in turn_pairs]

    def move(values, some):
        return lax.ppermute(values, axes, some)

    def place():
        row, col = lax.axis_index("row"), lax.axis_index("col")
        return row % 2, col % groups

    def reorder(pieces):
        _, g = place()
        bit = 1
        while bit < groups:
            on = (g & bit) != 0
            pieces = [jnp.where(on, pieces[k ^ bit], pieces[k]) for k in range(groups)]
            bit *= 2
        return pieces

    def split(values, count):
        span = values.shape[-1] // count
        return [values[..., i * span : (i + 1) * span] for i in range(count)]

    def to_pieces(own, mates):
        core, _ = place()
        first, second = jnp.where(core == 0, own, mates), jnp.where(core == 0, mates, own)
        return reorder(split(first, top) + split(second, top))

    def from_pieces(pieces):
        core, _ = place()
        pieces = reorder(pieces)
        first = jnp.concatenate(pieces[:top], axis=-1)
        second = jnp.concatenate(pieces[top:], axis=-1)
        return jnp.where(core == 0, first, second), jnp.where(core == 0, second, first)

    def call(kernel, name, outs, args, flops):
        shapes = [jax.ShapeDtypeStruct(s, jnp.float32) for s in outs]
        return pl.pallas_call(
            kernel,
            out_shape=shapes,
            in_specs=[VMEM] * len(args),
            out_specs=[VMEM] * len(outs),
            name=name,
            cost_estimate=pl.CostEstimate(flops=flops, bytes_accessed=1 << 20, transcendentals=0),
            compiler_params=pltpu.CompilerParams(vmem_limit_bytes=8 << 20),
        )(*args)

    def limbs(own, mates, name):
        rows, span = own.shape[-2:]
        lead = own.shape[:-2]
        count = own.size // (rows * span)
        slots = 4

        def kernel(own_ref, mate_ref, large, small, buffer, done):
            core, g = place()

            def copies(i, slot):
                return [
                    pltpu.make_async_copy(ref.at[i], buffer.at[slot, s], done.at[slot, s])
                    for s, ref in enumerate((own_ref, mate_ref))
                ]

            for i in range(min(slots, count)):
                for copy in copies(i, i):
                    copy.start()

            def step(i, carry):
                slot = lax.rem(i, slots)
                for s, copy in enumerate(copies(i, slot)):
                    copy.wait()
                    side = core if s == 0 else 1 - core
                    for b in range(top):
                        at = (side * top + b) ^ g
                        values = buffer[slot, s, b * span : (b + 1) * span, :]
                        first = values.astype(jnp.bfloat16)
                        large[i, at] = first
                        small[i, at] = (values - first.astype(jnp.float32)).astype(jnp.bfloat16)

                @pl.when(i + slots < count)
                def _():
                    for copy in copies(i + slots, slot):
                        copy.start()

                return carry

            lax.fori_loop(0, count, step, 0)

        shape = jax.ShapeDtypeStruct((count, groups, span, span), jnp.bfloat16)
        found = pl.pallas_call(
            kernel,
            out_shape=[shape] * 2,
            in_specs=[pl.BlockSpec(memory_space=pl.ANY)] * 2,
            out_specs=[VMEM] * 2,
            scratch_shapes=[
                pltpu.VMEM((slots, 2, rows, span), jnp.float32),
                pltpu.SemaphoreType.DMA((slots, 2)),
            ],
            name=name,
            cost_estimate=pl.CostEstimate(
                flops=count << 24, bytes_accessed=count << 21, transcendentals=0
            ),
            compiler_params=pltpu.CompilerParams(vmem_limit_bytes=8 << 20),
        )(own.reshape(count, rows, span), mates.reshape(count, rows, span))
        return [values.reshape(*lead, groups * span, span) for values in found]

    def per_device(right_side, panels, diag_inverse, parents, live_width, tile_pattern):
        levels, per_level, rhs_count, row_span = right_side.shape
        col_span = panels.shape[3]
        half = rhs_count // 2
        row, col = lax.axis_index("row"), lax.axis_index("col")
        core, y = row % 2, row // 2
        piece = (per_level, half, col_span)
        work = 24 * per_level * half * row_span * col_span

        def live(first, span):
            cells = first + jnp.arange(span, dtype=jnp.int32)
            return (cells < live_width[:, :, None]).astype(jnp.float32)[:, :, None, :]

        order = jnp.arange(groups, dtype=jnp.int32) ^ place()[1]
        block_cells = (jnp.arange(col_span, dtype=jnp.int32) + col_span * order[:, None]).reshape(-1)
        row_cells = y * 2 * row_span + block_cells
        wide = (per_level, half, 2 * row_span)

        def live(cells):
            return (cells < live_width[:, :, None]).astype(jnp.float32)[:, :, None, :]

        col_live = live(col * col_span + jnp.arange(col_span, dtype=jnp.int32))
        row_live = live(row_cells)
        climbs = climb_maps(parents)
        climb_of = jnp.stack(
            [climbs[h, g] for h in range(levels) for g in range(h + 1, levels)]
        )
        tile_count = 2 * row_span // TILE
        tiles = lax.dynamic_slice_in_dim(tile_pattern, y * tile_count, tile_count, 2)
        keep = jnp.repeat(tiles.astype(jnp.float32), TILE, axis=2)
        keep = jnp.concatenate(reorder(split(keep, groups)), axis=-1)
        weight = (climb_of[:, :, :, None] * keep[:, :, None, :])[:, :, :, None, :]

        def down_diag(height, turned):
            def kernel(*refs):
                turned_refs, (mask, large, small), out = (
                    refs[:y_count],
                    refs[y_count : y_count + 3],
                    refs[y_count + 3 :],
                )
                for k in range(per_level):
                    x = sum(ref[k] for ref in turned_refs[1:]) + turned_refs[0][k]
                    x = x * mask[height, k]
                    pieces = split(product(x, large[height, k], small[height, k], 1), groups)
                    for i in range(groups):
                        out[i][k] = pieces[i]

            return call(
                kernel, f"down_diag_{height}", [piece] * groups, [*turned, col_live, *diag], work
            )

        def down_panel(height, turned, rest):
            slot = pair_index(height, height + 1, levels)

            def kernel(*refs):
                turned_refs = refs[:y_count]
                mask, weights, rest_ref, large, small = refs[y_count : y_count + 5]
                solved, out = refs[y_count + 5], refs[y_count + 6 :]
                left = [rest_ref[t] for t in range(per_level)]
                for k in range(per_level):
                    x = sum(ref[k] for ref in turned_refs[1:]) + turned_refs[0][k]
                    x = x * mask[height, k]
                    solved[k] = x
                    term = product(x, large[slot, k], small[slot, k], 1)
                    for t in range(per_level):
                        left[t] = left[t] - term * weights[slot, k, t]
                for t in range(per_level):
                    pieces = split(left[t], groups)
                    for i in range(groups):
                        out[i][t] = pieces[i]

            found = call(
                kernel,
                f"down_panel_{height}",
                [piece] * (groups + 1),
                [*turned, col_live, weight, rest, *blocks],
                work,
            )
            return found[0], found[1:]

        def down_rest(height, higher, solved, rest):
            slot = pair_index(height, higher, levels)

            def kernel(x_ref, weights, rest_ref, large, small, out):
                left = [rest_ref[t] for t in range(per_level)]
                for k in range(per_level):
                    term = product(x_ref[k], large[slot, k], small[slot, k], 1)
                    for t in range(per_level):
                        left[t] = left[t] - term * weights[slot, k, t]
                for t in range(per_level):
                    out[t] = left[t]

            return call(
                kernel,
                f"down_rest_{height}_{higher}",
                [wide],
                [solved, weight, rest, *blocks],
                work,
            )[0]

        def up_diag(height, received):
            def kernel(*refs):
                got = refs[:groups]
                mask, row_mask, large, small, out = refs[groups:]
                for k in range(per_level):
                    values = jnp.concatenate([ref[k] for ref in got], axis=-1)
                    values = values * row_mask[height, k]
                    out[k] = product(values, large[height, k], small[height, k], 0) * mask[height, k]

            return call(
                kernel,
                f"up_diag_{height}",
                [piece],
                [*received, col_live, row_live, *diag],
                work,
            )[0]

        def up_panel(height, received, rest):
            slot = pair_index(height, height + 1, levels)

            def kernel(*refs):
                got = refs[:groups]
                weights, rest_ref, large, small, out, found = refs[groups:]
                values = []
                for t in range(per_level):
                    values.append(jnp.concatenate([ref[t] for ref in got], axis=-1))
                    found[t] = values[t]
                for k in range(per_level):
                    part = sum(values[t] * weights[slot, k, t] for t in range(per_level))
                    out[k] = rest_ref[k] - product(part, large[slot, k], small[slot, k], 0)

            return call(
                kernel,
                f"up_panel_{height}",
                [piece, wide],
                [*received, weight, rest, *blocks],
                work,
            )

        def up_rest(height, higher, found, rest):
            slot = pair_index(height, higher, levels)

            def kernel(found_ref, weights, rest_ref, large, small, out):
                for k in range(per_level):
                    part = sum(found_ref[t] * weights[slot, k, t] for t in range(per_level))
                    out[k] = rest_ref[k] - product(part, large[slot, k], small[slot, k], 0)

            return call(
                kernel,
                f"up_rest_{height}_{higher}",
                [piece],
                [found, weight, rest, *blocks],
                work,
            )[0]

        def rows_to_cols(pieces):
            moved = [move(pieces[k], group_pairs[k]) for k in range(1, groups)]
            summed = sum(moved, pieces[0])
            return [move(summed, some) for some in turn_pairs]

        def spread(block):
            return [block] + [move(block, group_pairs[k]) for k in range(1, groups)]

        def cols_to_rows(values):
            turned = [move(values, some) for some in back_pairs]
            return spread(sum(turned[1:], turned[0]))

        def halves(values, which):
            return lax.dynamic_slice_in_dim(values, which * half, half, 2)

        def whole(own, mates):
            theirs = move(mates, swap_pairs)
            first, second = jnp.where(core == 0, own, theirs), jnp.where(core == 0, theirs, own)
            return jnp.concatenate([first, second], axis=2)

        own_side = halves(right_side, core)
        mate_side = move(halves(right_side, 1 - core), swap_pairs)
        diag = limbs(diag_inverse, move(diag_inverse, swap_pairs), "limbs_diag")
        blocks = limbs(panels, move(panels, swap_pairs), "limbs_panels")

        start = move(to_pieces(own_side[0], mate_side[0])[0], turn_pairs[0])
        once = (col == 0).astype(jnp.float32)
        side = jnp.concatenate(to_pieces(own_side[1:], mate_side[1:]), axis=-1) * once
        rest = [None] + [side[h] for h in range(levels - 1)]
        turned = [start] + [jnp.zeros_like(start)] * (y_count - 1)
        interim = []
        for height in range(levels):
            turned = rows_to_cols(down_diag(height, turned))
            if height + 1 < levels:
                solved, pieces = down_panel(height, turned, rest[height + 1])
                turned = rows_to_cols(pieces)
                for higher in range(height + 2, levels):
                    rest[higher] = down_rest(height, higher, solved, rest[higher])
            else:
                solved = sum(turned[1:], turned[0]) * col_live[height]
            interim.append(solved)

        received = spread(move(interim[levels - 1], back_pairs[0]))
        interim_own, interim_mate = from_pieces(spread(move(jnp.stack(interim), back_pairs[0])))
        interim_rows = whole(interim_own, interim_mate)

        first_y = (y == 0).astype(jnp.float32)
        rest = [values * first_y for values in interim]
        found = [None] * levels
        for height in reversed(range(levels)):
            received = cols_to_rows(up_diag(height, received))
            if height > 0:
                sent, found[height] = up_panel(height - 1, received, rest[height - 1])
                received = cols_to_rows(sent)
                for lower in range(height - 1):
                    rest[lower] = up_rest(lower, height, found[height], rest[lower])
            else:
                found[height] = jnp.concatenate(received, axis=-1)
        found_own, found_mate = from_pieces(split(jnp.stack(found), groups))
        return interim_rows, whole(found_own, found_mate)

    return jax.shard_map(
        per_device,
        mesh=mesh,
        in_specs=(
            P(None, None, None, "row"),
            P(None, None, "row", "col"),
            P(None, None, "row", "col"),
            P(),
            P(),
            P(),
        ),
        out_specs=(P(None, None, None, "row"), P(None, None, None, "row")),
        check_vma=False,
    )
```

```python
import jax
import jax.numpy as jnp
from jax import lax
from jax.experimental import pallas as pl
from jax.experimental.pallas import tpu as pltpu
from jax.sharding import PartitionSpec as P

TILE = 128


VMEM = pl.BlockSpec(memory_space=pltpu.VMEM)


def pair_index(lower, higher, depth_count):
    return lower * depth_count - lower * (lower + 1) // 2 + (higher - lower - 1)


def climb_maps(parents):
    depth_count, width_count = parents.shape[0] + 1, parents.shape[1]
    positions = jnp.arange(width_count, dtype=jnp.int32)
    climbs = {}
    for height in range(depth_count - 1):
        place = parents[height]
        climbs[height, height + 1] = (place[:, None] == positions).astype(jnp.float32)
        for higher in range(height + 2, depth_count):
            step = parents[higher - 1]
            place = sum(jnp.where(place == k, step[k], 0) for k in range(width_count))
            climbs[height, higher] = (place[:, None] == positions).astype(jnp.float32)
    return climbs


def limbs_of(values, count):
    parts = []
    rest = values
    for i in range(count):
        part = rest.astype(jnp.bfloat16)
        parts.append(part)
        if i + 1 < count:
            rest = rest - part.astype(jnp.float32)
    return parts


def product(values, large, small, contract_block):
    m = values.shape[0]
    left = limbs_of(values, 3)
    total = None
    for block, count in ((small, 2), (large, 3)):
        found = lax.dot_general(
            jnp.concatenate(left[:count], axis=0),
            block,
            (((1,), (contract_block,)), ((), ())),
            preferred_element_type=jnp.float32,
        )
        for n in reversed(range(count)):
            part = found[n * m : (n + 1) * m]
            total = part if total is None else total + part
    return total


def solution(mesh):
    row_count, col_count = mesh.shape["row"], mesh.shape["col"]
    y_count = row_count // 2
    groups = col_count // y_count
    assert row_count == 2 * y_count and col_count == groups * y_count
    assert groups >= 2 and groups & (groups - 1) == 0
    top = groups // 2
    axes = ("row", "col")

    def pairs(move):
        found = []
        for row in range(row_count):
            for col in range(col_count):
                y, core, q, g = move(row // 2, row % 2, col // groups, col % groups)
                found.append((row * col_count + col, (2 * y + core) * col_count + groups * q + g))
        return found

    swap_pairs = pairs(lambda y, core, q, g: (y, 1 - core, q, g))
    group_pairs = [pairs(lambda y, core, q, g, k=k: (y, core, q, g ^ k)) for k in range(groups)]
    turn_pairs = [
        pairs(lambda y, core, q, g, t=t: ((q + t) % y_count, core, y, g)) for t in range(y_count)
    ]
    cross_pairs = [
        pairs(lambda y, core, q, g, t=t: (y, core, (t - q) % y_count, g)) for t in range(y_count)
    ]
    back_pairs = [[(b, a) for a, b in some] for some in turn_pairs]

    def move(values, some):
        return lax.ppermute(values, axes, some)

    def place():
        row, col = lax.axis_index("row"), lax.axis_index("col")
        return row % 2, col % groups

    def reorder(pieces):
        _, g = place()
        bit = 1
        while bit < groups:
            on = (g & bit) != 0
            pieces = [jnp.where(on, pieces[k ^ bit], pieces[k]) for k in range(groups)]
            bit *= 2
        return pieces

    def split(values, count):
        span = values.shape[-1] // count
        return [values[..., i * span : (i + 1) * span] for i in range(count)]

    def to_pieces(own, mates):
        core, _ = place()
        first, second = jnp.where(core == 0, own, mates), jnp.where(core == 0, mates, own)
        return reorder(split(first, top) + split(second, top))

    def from_pieces(pieces):
        core, _ = place()
        pieces = reorder(pieces)
        first = jnp.concatenate(pieces[:top], axis=-1)
        second = jnp.concatenate(pieces[top:], axis=-1)
        return jnp.where(core == 0, first, second), jnp.where(core == 0, second, first)

    def call(kernel, name, outs, args, flops):
        shapes = [jax.ShapeDtypeStruct(s, jnp.float32) for s in outs]
        return pl.pallas_call(
            kernel,
            out_shape=shapes,
            in_specs=[VMEM] * len(args),
            out_specs=[VMEM] * len(outs),
            name=name,
            cost_estimate=pl.CostEstimate(flops=flops, bytes_accessed=1 << 20, transcendentals=0),
            compiler_params=pltpu.CompilerParams(vmem_limit_bytes=8 << 20),
        )(*args)

    def limbs(own, mates, begin, end, name):
        rows, span = own.shape[-2:]
        per = own.shape[1]
        count = (end - begin) * per
        slots = min(4, count)

        def kernel(own_ref, mate_ref, large, small, buffer, done):
            core, g = place()

            def copies(i, slot):
                return [
                    pltpu.make_async_copy(ref.at[begin * per + i], buffer.at[slot, s], done.at[slot, s])
                    for s, ref in enumerate((own_ref, mate_ref))
                ]

            for i in range(slots):
                for copy in copies(i, i):
                    copy.start()

            def step(i, carry):
                slot = lax.rem(i, slots)
                for s, copy in enumerate(copies(i, slot)):
                    copy.wait()
                    side = core if s == 0 else 1 - core
                    for b in range(top):
                        at = (side * top + b) ^ g
                        values = buffer[slot, s, b * span : (b + 1) * span, :]
                        first = values.astype(jnp.bfloat16)
                        large[i, at] = first
                        small[i, at] = (values - first.astype(jnp.float32)).astype(jnp.bfloat16)

                @pl.when(i + slots < count)
                def _():
                    for copy in copies(i + slots, slot):
                        copy.start()

                return carry

            lax.fori_loop(0, count, step, 0)

        shape = jax.ShapeDtypeStruct((count, groups, span, span), jnp.bfloat16)
        found = pl.pallas_call(
            kernel,
            out_shape=[shape] * 2,
            in_specs=[pl.BlockSpec(memory_space=pl.ANY)] * 2,
            out_specs=[VMEM] * 2,
            scratch_shapes=[
                pltpu.VMEM((slots, 2, rows, span), jnp.float32),
                pltpu.SemaphoreType.DMA((slots, 2)),
            ],
            name=name,
            cost_estimate=pl.CostEstimate(
                flops=count << 24, bytes_accessed=count << 21, transcendentals=0
            ),
            compiler_params=pltpu.CompilerParams(vmem_limit_bytes=8 << 20),
        )(own.reshape(-1, rows, span), mates.reshape(-1, rows, span))
        return [values.reshape(end - begin, per, groups * span, span) for values in found]

    def rows_of(items, name):
        flat = [array for item in items for array in item]
        per, half = flat[0].shape[-3:-1]
        width = items[0][0].shape[-1] * len(items[0])
        counts = [item[0].shape[0] if item[0].ndim == 4 else 1 for item in items]
        total = sum(counts)

        def kernel(*refs):
            own_out, mate_out = refs[-2:]
            at, level_at = 0, 0
            for item, count in zip(items, counts, strict=True):
                mine = refs[at : at + len(item)]
                at += len(item)
                for n in range(count):
                    for k in range(per):
                        values = [ref[n, k] if ref.ndim == 4 else ref[k] for ref in mine]
                        if len(values) == 1:
                            values = split(values[0], groups)
                        own, mates = from_pieces(values)
                        own_out[level_at, k] = own
                        mate_out[level_at, k] = mates
                    level_at += 1

        return call(kernel, name, [(total, per, half, width // 2)] * 2, flat, 1000)

    def assemble(owns, theirs, name):
        per, half, span = owns[0].shape[-3:]
        total = sum(array.shape[0] for array in owns)

        def kernel(*refs):
            out = refs[-1]
            core, _ = place()
            for side, mine in ((core, refs[: len(owns)]), (1 - core, refs[len(owns) : -1])):
                rows = pl.ds(pl.multiple_of(side * half, half), half)
                at = 0
                for ref in mine:
                    for n in range(ref.shape[0]):
                        for k in range(per):
                            out[at, k, rows, :] = ref[n, k]
                        at += 1

        return call(kernel, name, [(total, per, 2 * half, span)], [*owns, *theirs], 1000)[0]

    def per_device(right_side, panels, diag_inverse, parents, live_width, tile_pattern):
        levels, per_level, rhs_count, row_span = right_side.shape
        col_span = panels.shape[3]
        half = rhs_count // 2
        row, col = lax.axis_index("row"), lax.axis_index("col")
        core, y = row % 2, row // 2
        piece = (per_level, half, col_span)
        work = 24 * per_level * half * row_span * col_span

        def live(first, span):
            cells = first + jnp.arange(span, dtype=jnp.int32)
            return (cells < live_width[:, :, None]).astype(jnp.float32)[:, :, None, :]

        order = jnp.arange(groups, dtype=jnp.int32) ^ place()[1]
        block_cells = (jnp.arange(col_span, dtype=jnp.int32) + col_span * order[:, None]).reshape(-1)
        row_cells = y * 2 * row_span + block_cells
        wide = (per_level, half, 2 * row_span)

        def live(cells):
            return (cells < live_width[:, :, None]).astype(jnp.float32)[:, :, None, :]

        col_live = live(col * col_span + jnp.arange(col_span, dtype=jnp.int32))
        row_live = live(row_cells)
        climbs = climb_maps(parents)
        climb_of = jnp.stack(
            [climbs[h, g] for h in range(levels) for g in range(h + 1, levels)]
        )
        tile_count = 2 * row_span // TILE
        tiles = lax.dynamic_slice_in_dim(tile_pattern, y * tile_count, tile_count, 2)
        keep = jnp.repeat(tiles.astype(jnp.float32), TILE, axis=2)
        keep = jnp.concatenate(reorder(split(keep, groups)), axis=-1)
        weight = (climb_of[:, :, :, None] * keep[:, :, None, :])[:, :, :, None, :]

        def down_diag(height, turned):
            at = 0 if height == 0 else height - 1

            def kernel(*refs):
                turned_refs, (mask, large, small), out = (
                    refs[:y_count],
                    refs[y_count : y_count + 3],
                    refs[y_count + 3 :],
                )
                for k in range(per_level):
                    x = sum(ref[k] for ref in turned_refs[1:]) + turned_refs[0][k]
                    x = x * mask[height, k]
                    pieces = split(product(x, large[at, k], small[at, k], 1), groups)
                    for i in range(groups):
                        out[i][k] = pieces[i]

            return call(
                kernel, f"down_diag_{height}", [piece] * groups, [*turned, col_live, *diag_of(height)], work
            )

        def down_panel(height, turned, rest):
            slot = pair_index(height, height + 1, levels)
            at = 0 if slot == 0 else slot - 1

            def kernel(*refs):
                turned_refs = refs[:y_count]
                mask, weights, rest_ref, large, small = refs[y_count : y_count + 5]
                solved, out = refs[y_count + 5], refs[y_count + 6 :]
                left = [rest_ref[t] for t in range(per_level)]
                for k in range(per_level):
                    x = sum(ref[k] for ref in turned_refs[1:]) + turned_refs[0][k]
                    x = x * mask[height, k]
                    solved[k] = x
                    term = product(x, large[at, k], small[at, k], 1)
                    for t in range(per_level):
                        left[t] = left[t] - term * weights[slot, k, t]
                for t in range(per_level):
                    pieces = split(left[t], groups)
                    for i in range(groups):
                        out[i][t] = pieces[i]

            found = call(
                kernel,
                f"down_panel_{height}",
                [piece] * (groups + 1),
                [*turned, col_live, weight, rest, *blocks_of(slot)],
                work,
            )
            return found[0], found[1:]

        def down_rest(height, higher, solved, rest):
            slot = pair_index(height, higher, levels)
            at = 0 if slot == 0 else slot - 1

            def kernel(x_ref, weights, rest_ref, large, small, out):
                left = [rest_ref[t] for t in range(per_level)]
                for k in range(per_level):
                    term = product(x_ref[k], large[at, k], small[at, k], 1)
                    for t in range(per_level):
                        left[t] = left[t] - term * weights[slot, k, t]
                for t in range(per_level):
                    out[t] = left[t]

            return call(
                kernel,
                f"down_rest_{height}_{higher}",
                [wide],
                [solved, weight, rest, *blocks_of(slot)],
                work,
            )[0]

        def up_diag(height, received):
            at = 0 if height == 0 else height - 1

            def kernel(*refs):
                got = refs[:groups]
                mask, row_mask, large, small, out = refs[groups:]
                for k in range(per_level):
                    values = jnp.concatenate([ref[k] for ref in got], axis=-1)
                    values = values * row_mask[height, k]
                    out[k] = product(values, large[at, k], small[at, k], 0) * mask[height, k]

            return call(
                kernel,
                f"up_diag_{height}",
                [piece],
                [*received, col_live, row_live, *diag_of(height)],
                work,
            )[0]

        def only_first_y(values, fresh):
            if not fresh:
                return values
            return jnp.where(lax.axis_index("row") // 2 == 0, values, jnp.zeros_like(values))

        def up_panel(height, received, rest, fresh):
            slot = pair_index(height, height + 1, levels)
            at = 0 if slot == 0 else slot - 1

            def kernel(*refs):
                got = refs[:groups]
                weights, rest_ref, large, small, out, found = refs[groups:]
                values = []
                for t in range(per_level):
                    values.append(jnp.concatenate([ref[t] for ref in got], axis=-1))
                    found[t] = values[t]
                for k in range(per_level):
                    part = sum(values[t] * weights[slot, k, t] for t in range(per_level))
                    out[k] = only_first_y(rest_ref[k], fresh) - product(part, large[at, k], small[at, k], 0)

            return call(
                kernel,
                f"up_panel_{height}",
                [piece, wide],
                [*received, weight, rest, *blocks_of(slot)],
                work,
            )

        def up_rest(height, higher, found, rest, fresh):
            slot = pair_index(height, higher, levels)
            at = 0 if slot == 0 else slot - 1

            def kernel(found_ref, weights, rest_ref, large, small, out):
                for k in range(per_level):
                    part = sum(found_ref[t] * weights[slot, k, t] for t in range(per_level))
                    out[k] = only_first_y(rest_ref[k], fresh) - product(part, large[at, k], small[at, k], 0)

            return call(
                kernel,
                f"up_rest_{height}_{higher}",
                [piece],
                [found, weight, rest, *blocks_of(slot)],
                work,
            )[0]

        def rows_to_cols(pieces):
            moved = [move(pieces[k], group_pairs[k]) for k in range(1, groups)]
            summed = sum(moved, pieces[0])
            return [move(summed, some) for some in turn_pairs]

        def spread(block):
            return [block] + [move(block, group_pairs[k]) for k in range(1, groups)]

        def cols_to_rows(values):
            turned = [move(values, some) for some in back_pairs]
            return spread(sum(turned[1:], turned[0]))

        def swap(values):
            return move(values, swap_pairs)

        def opening(side_ref, own_first, mate_first, own_rest, mate_rest):
            mine = place()[0]
            for which, first, others in ((mine, own_first, own_rest), (1 - mine, mate_first, mate_rest)):
                rows = pl.ds(pl.multiple_of(which * half, half), half)
                for k in range(per_level):
                    first[k] = side_ref[0, k, rows, :]
                    for h in range(1, levels):
                        others[h - 1, k] = side_ref[h, k, rows, :]

        one, rest_shape = (per_level, half, row_span), (levels - 1, per_level, half, row_span)
        own_first, give_first, own_others, give_others = call(
            opening, "opening", [one, one, rest_shape, rest_shape], [right_side], 1000
        )

        def first_piece(own_ref, mate_ref, out):
            for k in range(per_level):
                out[k] = to_pieces(own_ref[k], mate_ref[k])[0]

        def side_pieces(own_ref, mate_ref, *out):
            for h in range(levels - 1):
                for k in range(per_level):
                    values = jnp.concatenate(to_pieces(own_ref[h, k], mate_ref[h, k]), axis=-1)
                    out[h][k] = jnp.where(lax.axis_index("col") == 0, values, jnp.zeros_like(values))

        mate_first = swap(give_first)
        mate_first, diag_sent, give_others = lax.optimization_barrier(
            (mate_first, diag_inverse, give_others)
        )
        start = call(first_piece, "first_piece", [piece], [own_first, mate_first], 1000)[0]
        start = move(start, turn_pairs[0])
        mate_diag = swap(diag_sent)
        mate_diag, panels_sent, give_others, col_live, row_live, weight = lax.optimization_barrier(
            (mate_diag, panels, give_others, col_live, row_live, weight)
        )
        mate_others = swap(give_others)
        mate_panels = swap(panels_sent)
        diag_first = limbs(diag_inverse, mate_diag, 0, 1, "limbs_diag_first")
        diag_rest = limbs(diag_inverse, mate_diag, 1, levels, "limbs_diag_rest")
        pair_count = levels * (levels - 1) // 2
        blocks_first = limbs(panels, mate_panels, 0, 1, "limbs_panels_first")
        blocks_rest = limbs(panels, mate_panels, 1, pair_count, "limbs_panels_rest")

        def diag_of(height):
            return diag_first if height == 0 else diag_rest

        def blocks_of(slot):
            return blocks_first if slot == 0 else blocks_rest

        rest = [None, *call(side_pieces, "side", [wide] * (levels - 1), [own_others, mate_others], 1000)]
        turned = [start] + [jnp.zeros_like(start)] * (y_count - 1)
        interim = []
        for height in range(levels - 1):
            turned = rows_to_cols(down_diag(height, turned))
            solved, pieces = down_panel(height, turned, rest[height + 1])
            turned = rows_to_cols(pieces)
            for higher in range(height + 2, levels):
                rest[higher] = down_rest(height, higher, solved, rest[higher])
            interim.append(solved)

        pieces = down_diag(levels - 1, turned)
        moved = [move(pieces[k], group_pairs[k]) for k in range(1, groups)]
        summed = sum(moved, pieces[0])
        crossed = [move(summed, some) for some in cross_pairs]
        top_rows = received = spread(sum(crossed[1:], crossed[0]))

        found = [None] * levels
        rest = list(interim)
        for height in reversed(range(levels)):
            received = cols_to_rows(up_diag(height, received))
            if height > 0:
                fresh = height == levels - 1
                sent, found[height] = up_panel(height - 1, received, rest[height - 1], fresh)
                received = cols_to_rows(sent)
                for lower in range(height - 1):
                    rest[lower] = up_rest(lower, height, found[height], rest[lower], fresh)

        def top_mask(*refs):
            got, mask, out = refs[:groups], refs[groups], refs[groups + 1]
            for k in range(per_level):
                values = jnp.concatenate([ref[k] for ref in got], axis=-1)
                out[k] = values * mask[levels - 1, k]

        lower_rows = spread(move(jnp.stack(interim), back_pairs[0]))
        top_wide = call(top_mask, "top_mask", [wide], [*top_rows, row_live], 1000)
        own, mates = rows_of([lower_rows, top_wide], "interim_rows")
        interim_rows = assemble([own], [swap(mates)], "interim_out")

        own_higher, mate_higher = rows_of([[values] for values in found[1:]], "found_rows")
        theirs_higher = swap(mate_higher)
        own_lowest, mate_lowest = rows_of([received], "lowest_rows")
        solution_rows = assemble(
            [own_lowest, own_higher], [swap(mate_lowest), theirs_higher], "found_out"
        )
        return interim_rows, solution_rows

    return jax.shard_map(
        per_device,
        mesh=mesh,
        in_specs=(
            P(None, None, None, "row"),
            P(None, None, "row", "col"),
            P(None, None, "row", "col"),
            P(),
            P(),
            P(),
        ),
        out_specs=(P(None, None, None, "row"), P(None, None, None, "row")),
        check_vma=False,
    )
```

```python
import jax
import jax.numpy as jnp
from jax import lax
from jax.experimental import pallas as pl
from jax.experimental.pallas import tpu as pltpu
from jax.sharding import PartitionSpec as P


TILE = 128


VMEM = pl.BlockSpec(memory_space=pltpu.VMEM)
SMEM = pl.BlockSpec(memory_space=pltpu.SMEM)
HBM = pl.BlockSpec(memory_space=pltpu.HBM)


def pair_index(lower, higher, depth_count):
    return lower * depth_count - lower * (lower + 1) // 2 + (higher - lower - 1)


def limbs_of(values, count):
    parts = []
    rest = values
    for i in range(count):
        part = rest.astype(jnp.bfloat16)
        parts.append(part)
        if i + 1 < count:
            rest = rest - part.astype(jnp.float32)
    return parts


def product(values, large, small, contract_block):
    m = values.shape[0]
    left = limbs_of(values, 3)
    total = None
    for block, count in ((small, 2), (large, 3)):
        found = lax.dot_general(
            jnp.concatenate(left[:count], axis=0),
            block,
            (((1,), (contract_block,)), ((), ())),
            preferred_element_type=jnp.float32,
        )
        for n in reversed(range(count)):
            part = found[n * m : (n + 1) * m]
            total = part if total is None else total + part
    return total


def solution(mesh):
    row_count, col_count = mesh.shape["row"], mesh.shape["col"]
    y_count = row_count // 2
    groups = col_count // y_count
    assert row_count == 2 * y_count and col_count == groups * y_count
    assert groups >= 2 and groups & (groups - 1) == 0
    top = groups // 2
    axes = ("row", "col")

    def pairs(move):
        found = []
        for row in range(row_count):
            for col in range(col_count):
                y, core, q, g = move(row // 2, row % 2, col // groups, col % groups)
                found.append((row * col_count + col, (2 * y + core) * col_count + groups * q + g))
        return found

    swap_pairs = pairs(lambda y, core, q, g: (y, 1 - core, q, g))
    group_pairs = [pairs(lambda y, core, q, g, k=k: (y, core, q, g ^ k)) for k in range(groups)]
    turn_pairs = [
        pairs(lambda y, core, q, g, t=t: ((q + t) % y_count, core, y, g)) for t in range(y_count)
    ]
    cross_pairs = [
        pairs(lambda y, core, q, g, t=t: (y, core, (t - q) % y_count, g)) for t in range(y_count)
    ]
    back_pairs = [[(b, a) for a, b in some] for some in turn_pairs]

    def move(values, some):
        return lax.ppermute(values, axes, some)

    def place():
        row, col = lax.axis_index("row"), lax.axis_index("col")
        return row % 2, col % groups

    def reorder(pieces):
        _, g = place()
        bit = 1
        while bit < groups:
            on = (g & bit) != 0
            pieces = [jnp.where(on, pieces[k ^ bit], pieces[k]) for k in range(groups)]
            bit *= 2
        return pieces

    def split(values, count):
        span = values.shape[-1] // count
        return [values[..., i * span : (i + 1) * span] for i in range(count)]

    def to_pieces(own, mates):
        core, _ = place()
        first, second = jnp.where(core == 0, own, mates), jnp.where(core == 0, mates, own)
        return reorder(split(first, top) + split(second, top))

    def from_pieces(pieces):
        core, _ = place()
        pieces = reorder(pieces)
        first = jnp.concatenate(pieces[:top], axis=-1)
        second = jnp.concatenate(pieces[top:], axis=-1)
        return jnp.where(core == 0, first, second), jnp.where(core == 0, second, first)

    def call(kernel, outs, args, flops, space=VMEM):
        shapes = [jax.ShapeDtypeStruct(s, jnp.float32) for s in outs]
        return pl.pallas_call(
            kernel,
            out_shape=shapes,
            in_specs=[space] * len(args),
            out_specs=[VMEM] * len(outs),
            cost_estimate=pl.CostEstimate(flops=flops, bytes_accessed=1 << 20, transcendentals=0),
            compiler_params=pltpu.CompilerParams(vmem_limit_bytes=8 << 20),
        )(*args)

    def limbs(own, mates, begin, end, limit=8):
        rows, span = own.shape[-2:]
        per = own.shape[1]
        count = (end - begin) * per
        slots = min(4, count)

        def kernel(own_ref, mate_ref, large, small, buffer, done):
            core, g = place()

            def copies(i, slot):
                return [
                    pltpu.make_async_copy(ref.at[begin * per + i], buffer.at[slot, s], done.at[slot, s])
                    for s, ref in enumerate((own_ref, mate_ref))
                ]

            for i in range(slots):
                for copy in copies(i, i):
                    copy.start()

            def step(i, carry):
                slot = lax.rem(i, slots)
                for s, copy in enumerate(copies(i, slot)):
                    copy.wait()
                    side = core if s == 0 else 1 - core
                    for b in range(top):
                        at = (side * top + b) ^ g
                        values = buffer[slot, s, b * span : (b + 1) * span, :]
                        first = values.astype(jnp.bfloat16)
                        large[i, at] = first
                        small[i, at] = (values - first.astype(jnp.float32)).astype(jnp.bfloat16)

                @pl.when(i + slots < count)
                def _():
                    for copy in copies(i + slots, slot):
                        copy.start()

                return carry

            lax.fori_loop(0, count, step, 0)

        shape = jax.ShapeDtypeStruct((count, groups, span, span), jnp.bfloat16)
        found = pl.pallas_call(
            kernel,
            out_shape=[shape] * 2,
            in_specs=[HBM] * 2,
            out_specs=[VMEM] * 2,
            scratch_shapes=[
                pltpu.VMEM((slots, 2, rows, span), jnp.float32),
                pltpu.SemaphoreType.DMA((slots, 2)),
            ],
            cost_estimate=pl.CostEstimate(
                flops=count << 24, bytes_accessed=count << 21, transcendentals=0
            ),
            compiler_params=pltpu.CompilerParams(vmem_limit_bytes=limit << 20),
        )(own.reshape(-1, rows, span), mates.reshape(-1, rows, span))
        return [values.reshape(end - begin, per, groups * span, span) for values in found]

    def rows_of(items):
        flat = [array for item in items for array in item]
        per, half = flat[0].shape[-3:-1]
        width = items[0][0].shape[-1] * len(items[0])
        counts = [item[0].shape[0] if item[0].ndim == 4 else 1 for item in items]
        total = sum(counts)

        def kernel(*refs):
            own_out, mate_out = refs[-2:]
            at, level_at = 0, 0
            for item, count in zip(items, counts, strict=True):
                mine = refs[at : at + len(item)]
                at += len(item)
                for n in range(count):
                    for k in range(per):
                        values = [ref[n, k] if ref.ndim == 4 else ref[k] for ref in mine]
                        if len(values) == 1:
                            values = split(values[0], groups)
                        own, mates = from_pieces(values)
                        own_out[level_at, k] = own
                        mate_out[level_at, k] = mates
                    level_at += 1

        return call(kernel, [(total, per, half, width // 2)] * 2, flat, 1000)

    def assemble(owns, theirs):
        per, half, span = owns[0].shape[-3:]
        total = sum(array.shape[0] for array in owns)

        def kernel(*refs):
            out = refs[-1]
            core, _ = place()
            for side, mine in ((core, refs[: len(owns)]), (1 - core, refs[len(owns) : -1])):
                rows = pl.ds(pl.multiple_of(side * half, half), half)
                at = 0
                for ref in mine:
                    for n in range(ref.shape[0]):
                        for k in range(per):
                            out[at, k, rows, :] = ref[n, k]
                        at += 1

        return call(kernel, [(total, per, 2 * half, span)], [*owns, *theirs], 1000)[0]

    def per_device(right_side, panels, diag_inverse, parents, live_width, tile_pattern):
        levels, per_level, rhs_count, row_span = right_side.shape
        col_span = panels.shape[3]
        half = rhs_count // 2
        piece = (per_level, half, col_span)
        work = 24 * per_level * half * row_span * col_span

        wide = (per_level, half, 2 * row_span)
        pair_list = [(h, g) for h in range(levels) for g in range(h + 1, levels)]

        def setup(parents_ref, width_ref, tiles_ref, col_out, row_out, weight_out):
            _, g = place()
            y_at, col_at = lax.axis_index("row") // 2, lax.axis_index("col")
            cells = lax.broadcasted_iota(jnp.int32, (1, col_span), 1)
            for h in range(levels):
                for k in range(per_level):
                    left = width_ref[h, k] - col_at * col_span
                    col_out[h, k] = jnp.where(cells < left, 1.0, 0.0)
                    for i in range(groups):
                        left = width_ref[h, k] - y_at * 2 * row_span - (g ^ i) * col_span
                        at = pl.ds(i * col_span, col_span)
                        row_out[h, k, :, at] = jnp.where(cells < left, 1.0, 0.0)
            per_group = col_span // TILE
            for slot, (low, high) in enumerate(pair_list):
                for k in range(per_level):
                    above = parents_ref[low, k]
                    for step in range(low + 1, high):
                        above = parents_ref[step, above]
                    for i in range(groups):
                        first = (y_at * groups + (g ^ i)) * per_group
                        for n in range(per_group):
                            present = tiles_ref[slot, k, first + n]
                            at = pl.ds(i * col_span + n * TILE, TILE)
                            for t in range(per_level):
                                kept = jnp.where(above == t, present, 0)
                                value = jnp.full((1, TILE), kept, jnp.int32)
                                weight_out[slot, k, t, :, at] = value.astype(jnp.float32)

        col_live, row_live, weight = call(
            setup,
            [
                (levels, per_level, 1, col_span),
                (levels, per_level, 1, 2 * row_span),
                (len(pair_list), per_level, per_level, 1, 2 * row_span),
            ],
            [parents, live_width, tile_pattern],
            1000,
            SMEM,
        )

        def down_diag(height, turned):
            at = 0 if height == 0 else height - 1

            def kernel(*refs):
                turned_refs, (mask, large, small), out = (
                    refs[:y_count],
                    refs[y_count : y_count + 3],
                    refs[y_count + 3 :],
                )
                for k in range(per_level):
                    x = sum(ref[k] for ref in turned_refs[1:]) + turned_refs[0][k]
                    x = x * mask[height, k]
                    pieces = split(product(x, large[at, k], small[at, k], 1), groups)
                    for i in range(groups):
                        out[i][k] = pieces[i]

            return call(kernel, [piece] * groups, [*turned, col_live, *diag_of(height)], work)

        def down_panel(height, turned, rest):
            slot = pair_index(height, height + 1, levels)
            at = slot if slot == 0 else slot - 1 if slot < levels else slot - levels

            def kernel(*refs):
                turned_refs = refs[:y_count]
                mask, weights, rest_ref, large, small = refs[y_count : y_count + 5]
                solved, out = refs[y_count + 5], refs[y_count + 6 :]
                left = [rest_ref[t] for t in range(per_level)]
                for k in range(per_level):
                    x = sum(ref[k] for ref in turned_refs[1:]) + turned_refs[0][k]
                    x = x * mask[height, k]
                    solved[k] = x
                    term = product(x, large[at, k], small[at, k], 1)
                    for t in range(per_level):
                        left[t] = left[t] - term * weights[slot, k, t]
                for t in range(per_level):
                    pieces = split(left[t], groups)
                    for i in range(groups):
                        out[i][t] = pieces[i]

            found = call(
                kernel,
                [piece] * (groups + 1),
                [*turned, col_live, weight, rest, *blocks_of(slot)],
                work,
            )
            return found[0], found[1:]

        def down_rest(height, higher, solved, rest):
            slot = pair_index(height, higher, levels)
            at = slot if slot == 0 else slot - 1 if slot < levels else slot - levels

            def kernel(x_ref, weights, rest_ref, large, small, out):
                left = [rest_ref[t] for t in range(per_level)]
                for k in range(per_level):
                    term = product(x_ref[k], large[at, k], small[at, k], 1)
                    for t in range(per_level):
                        left[t] = left[t] - term * weights[slot, k, t]
                for t in range(per_level):
                    out[t] = left[t]

            return call(kernel, [wide], [solved, weight, rest, *blocks_of(slot)], work)[0]

        def up_diag(height, received):
            at = 0 if height == 0 else height - 1

            def kernel(*refs):
                got = refs[:groups][::-1]
                mask, row_mask, large, small, out = refs[groups:]
                for k in range(per_level):
                    values = jnp.concatenate([ref[k] for ref in got], axis=-1)
                    values = values * row_mask[height, k]
                    out[k] = product(values, large[at, k], small[at, k], 0) * mask[height, k]

            return call(
                kernel, [piece], [*received[::-1], col_live, row_live, *diag_of(height)], work
            )[0]

        def only_first_y(values, fresh):
            if not fresh:
                return values
            return jnp.where(lax.axis_index("row") // 2 == 0, values, jnp.zeros_like(values))

        def up_panel(height, received, rest, fresh):
            slot = pair_index(height, height + 1, levels)
            at = slot if slot == 0 else slot - 1 if slot < levels else slot - levels

            def kernel(*refs):
                got = refs[:groups][::-1]
                weights, rest_ref, large, small, out, found = refs[groups:]
                values = []
                for t in range(per_level):
                    values.append(jnp.concatenate([ref[t] for ref in got], axis=-1))
                    found[t] = values[t]
                for k in range(per_level):
                    part = sum(values[t] * weights[slot, k, t] for t in range(per_level))
                    out[k] = only_first_y(rest_ref[k], fresh) - product(part, large[at, k], small[at, k], 0)

            return call(
                kernel, [piece, wide], [*received[::-1], weight, rest, *blocks_of(slot)], work
            )

        def up_rest(height, higher, found, rest, fresh):
            slot = pair_index(height, higher, levels)
            at = slot if slot == 0 else slot - 1 if slot < levels else slot - levels

            def kernel(found_ref, weights, rest_ref, large, small, out):
                for k in range(per_level):
                    part = sum(found_ref[t] * weights[slot, k, t] for t in range(per_level))
                    out[k] = only_first_y(rest_ref[k], fresh) - product(part, large[at, k], small[at, k], 0)

            return call(kernel, [piece], [found, weight, rest, *blocks_of(slot)], work)[0]

        def rows_to_cols(pieces):
            moved = [move(pieces[k], group_pairs[k]) for k in range(1, groups)]
            summed = sum(moved, pieces[0])
            return [move(summed, some) for some in turn_pairs[::-1]]

        def spread(block):
            return [block] + [move(block, group_pairs[k]) for k in range(1, groups)]

        def cols_to_rows(values):
            turned = [move(values, some) for some in back_pairs[::-1]]
            return spread(sum(turned[1:], turned[0]))

        def swap(values):
            return move(values, swap_pairs)

        def opening(side_ref, own_first, mate_first, own_rest, mate_rest):
            mine = place()[0]
            for which, first, others in ((mine, own_first, own_rest), (1 - mine, mate_first, mate_rest)):
                rows = pl.ds(pl.multiple_of(which * half, half), half)
                for k in range(per_level):
                    first[k] = side_ref[0, k, rows, :]
                    for h in range(1, levels):
                        others[h - 1, k] = side_ref[h, k, rows, :]

        one, rest_shape = (per_level, half, row_span), (levels - 1, per_level, half, row_span)
        own_first, give_first, own_others, give_others = call(
            opening, [one, one, rest_shape, rest_shape], [right_side], 1000
        )

        def first_piece(own_ref, mate_ref, out):
            for k in range(per_level):
                out[k] = to_pieces(own_ref[k], mate_ref[k])[0]

        def side_pieces(own_ref, mate_ref, *out):
            for h in range(levels - 1):
                for k in range(per_level):
                    values = jnp.concatenate(to_pieces(own_ref[h, k], mate_ref[h, k]), axis=-1)
                    out[h][k] = jnp.where(lax.axis_index("col") == 0, values, jnp.zeros_like(values))

        def take(diag_ref, block_ref, diag_out, block_out, done):
            copies = [
                pltpu.make_async_copy(ref.at[pl.ds(0, 1)], out, done.at[n])
                for n, (ref, out) in enumerate(((diag_ref, diag_out), (block_ref, block_out)))
            ]
            for copy in copies:
                copy.start()
            for copy in copies:
                copy.wait()

        mate_first = swap(give_first)
        head = jax.ShapeDtypeStruct((1, *diag_inverse.shape[1:]), jnp.float32)
        taken = pl.pallas_call(
            take,
            out_shape=[head] * 2,
            in_specs=[HBM] * 2,
            out_specs=[VMEM] * 2,
            scratch_shapes=[pltpu.SemaphoreType.DMA((2,))],
            name="take",
            cost_estimate=pl.CostEstimate(flops=1000, bytes_accessed=1 << 21, transcendentals=0),
            compiler_params=pltpu.CompilerParams(vmem_limit_bytes=60 << 20),
        )
        own_diag_first, own_block_first = taken(diag_inverse, panels)
        start = call(first_piece, [piece], [own_first, mate_first], 1000)[0]
        start = move(start, turn_pairs[0])
        mate_diag_first, mate_block_first = swap(own_diag_first), swap(own_block_first)
        mate_others = swap(give_others)
        diag_first = limbs(own_diag_first, mate_diag_first, 0, 1)
        blocks_first = limbs(own_block_first, mate_block_first, 0, 1)
        diag_first, blocks_first, diag_all, panels_all, col_live, row_live, weight = (
            lax.optimization_barrier(
                (
                    diag_first,
                    blocks_first,
                    diag_inverse,
                    panels,
                    col_live,
                    row_live,
                    weight,
                )
            )
        )
        mate_diag = swap(diag_all)
        mate_panels = swap(panels_all)
        diag_rest = limbs(diag_inverse, mate_diag, 1, levels)
        blocks_near = limbs(panels, mate_panels, 1, levels, 42)
        blocks_rest = limbs(panels, mate_panels, levels, len(pair_list))

        def diag_of(height):
            return diag_first if height == 0 else diag_rest

        def blocks_of(slot):
            return blocks_first if slot == 0 else blocks_near if slot < levels else blocks_rest

        rest = [None, *call(side_pieces, [wide] * (levels - 1), [own_others, mate_others], 1000)]
        turned = [start] + [jnp.zeros_like(start)] * (y_count - 1)
        interim = []
        for height in range(levels - 1):
            turned = rows_to_cols(down_diag(height, turned))
            solved, pieces = down_panel(height, turned, rest[height + 1])
            turned = rows_to_cols(pieces)
            for higher in range(height + 2, levels):
                rest[higher] = down_rest(height, higher, solved, rest[higher])
            interim.append(solved)

        pieces = down_diag(levels - 1, turned)
        moved = [move(pieces[k], group_pairs[k]) for k in range(1, groups)]
        summed = sum(moved, pieces[0])
        crossed = [move(summed, some) for some in cross_pairs]
        top_rows = received = spread(sum(crossed[1:], crossed[0]))

        found = [None] * levels
        rest = list(interim)
        for height in reversed(range(levels)):
            received = cols_to_rows(up_diag(height, received))
            if height > 0:
                fresh = height == levels - 1
                sent, found[height] = up_panel(height - 1, received, rest[height - 1], fresh)
                received = cols_to_rows(sent)
                for lower in range(height - 1):
                    rest[lower] = up_rest(lower, height, found[height], rest[lower], fresh)

        def top_mask(*refs):
            got, mask, out = refs[:groups][::-1], refs[groups], refs[groups + 1]
            for k in range(per_level):
                values = jnp.concatenate([ref[k] for ref in got], axis=-1)
                out[k] = values * mask[levels - 1, k]

        lower_rows = spread(move(jnp.stack(interim), back_pairs[0]))
        top_wide = call(top_mask, [wide], [*top_rows[::-1], row_live], 1000)
        own, mates = rows_of([lower_rows, top_wide])
        interim_rows = assemble([own], [swap(mates)])

        own_higher, mate_higher = rows_of([[values] for values in found[1:]])
        theirs_higher = swap(mate_higher)
        own_lowest, mate_lowest = rows_of([received])
        solution_rows = assemble([own_lowest, own_higher], [swap(mate_lowest), theirs_higher])
        return interim_rows, solution_rows

    return jax.shard_map(
        per_device,
        mesh=mesh,
        in_specs=(
            P(None, None, None, "row"),
            P(None, None, "row", "col"),
            P(None, None, "row", "col"),
            P(),
            P(),
            P(),
        ),
        out_specs=(P(None, None, None, "row"), P(None, None, None, "row")),
        check_vma=False,
    )
```

```python
import jax
import jax.numpy as jnp
from jax import lax
from jax.experimental import pallas as pl
from jax.experimental.pallas import tpu as pltpu
from jax.sharding import PartitionSpec as P


TILE = 128


VMEM = pl.BlockSpec(memory_space=pltpu.VMEM)
SMEM = pl.BlockSpec(memory_space=pltpu.SMEM)
HBM = pl.BlockSpec(memory_space=pltpu.HBM)


def pair_index(lower, higher, depth_count):
    return lower * depth_count - lower * (lower + 1) // 2 + (higher - lower - 1)


def limbs_of(values, count):
    parts = []
    rest = values
    for i in range(count):
        part = rest.astype(jnp.bfloat16)
        parts.append(part)
        if i + 1 < count:
            rest = rest - part.astype(jnp.float32)
    return parts


def product(values, large, small, contract_block):
    m = values.shape[0]
    left = limbs_of(values, 3)
    total = None
    for block, count in ((small, 2), (large, 3)):
        found = lax.dot_general(
            jnp.concatenate(left[:count], axis=0),
            block,
            (((1,), (contract_block,)), ((), ())),
            preferred_element_type=jnp.float32,
        )
        for n in reversed(range(count)):
            part = found[n * m : (n + 1) * m]
            total = part if total is None else total + part
    return total


def solution(mesh):
    row_count, col_count = mesh.shape["row"], mesh.shape["col"]
    y_count = row_count // 2
    groups = col_count // y_count
    assert row_count == 2 * y_count and col_count == groups * y_count
    assert groups >= 2 and groups & (groups - 1) == 0
    top = groups // 2
    axes = ("row", "col")

    def pairs(move):
        found = []
        for row in range(row_count):
            for col in range(col_count):
                y, core, q, g = move(row // 2, row % 2, col // groups, col % groups)
                found.append((row * col_count + col, (2 * y + core) * col_count + groups * q + g))
        return found

    swap_pairs = pairs(lambda y, core, q, g: (y, 1 - core, q, g))
    group_pairs = [pairs(lambda y, core, q, g, k=k: (y, core, q, g ^ k)) for k in range(groups)]
    turn_pairs = [
        pairs(lambda y, core, q, g, t=t: ((q + t) % y_count, core, y, g)) for t in range(y_count)
    ]
    cross_pairs = [
        pairs(lambda y, core, q, g, t=t: (y, core, (q + t) % y_count, g))
        for t in range(1, y_count)
    ]
    back_pairs = [[(b, a) for a, b in some] for some in turn_pairs]

    def move(values, some):
        return lax.ppermute(values, axes, some)

    def place():
        row, col = lax.axis_index("row"), lax.axis_index("col")
        return row % 2, col % groups

    def reorder(pieces):
        _, g = place()
        bit = 1
        while bit < groups:
            on = (g & bit) != 0
            pieces = [jnp.where(on, pieces[k ^ bit], pieces[k]) for k in range(groups)]
            bit *= 2
        return pieces

    def split(values, count):
        span = values.shape[-1] // count
        return [values[..., i * span : (i + 1) * span] for i in range(count)]

    def to_pieces(own, mates):
        core, _ = place()
        first, second = jnp.where(core == 0, own, mates), jnp.where(core == 0, mates, own)
        return reorder(split(first, top) + split(second, top))

    def from_pieces(pieces):
        core, _ = place()
        pieces = reorder(pieces)
        first = jnp.concatenate(pieces[:top], axis=-1)
        second = jnp.concatenate(pieces[top:], axis=-1)
        return jnp.where(core == 0, first, second), jnp.where(core == 0, second, first)

    def call(kernel, outs, args, flops, space=VMEM):
        shapes = [jax.ShapeDtypeStruct(s, jnp.float32) for s in outs]
        return pl.pallas_call(
            kernel,
            out_shape=shapes,
            in_specs=[space] * len(args),
            out_specs=[VMEM] * len(outs),
            cost_estimate=pl.CostEstimate(flops=flops, bytes_accessed=1 << 20, transcendentals=0),
            compiler_params=pltpu.CompilerParams(vmem_limit_bytes=8 << 20),
        )(*args)

    def limbs(own, mates, begin, end, limit=8):
        rows, span = own.shape[-2:]
        per = own.shape[1]
        count = (end - begin) * per
        slots = min(4, count)

        def kernel(own_ref, mate_ref, large, small, buffer, done):
            core, g = place()

            def copies(i, slot):
                return [
                    pltpu.make_async_copy(ref.at[begin * per + i], buffer.at[slot, s], done.at[slot, s])
                    for s, ref in enumerate((own_ref, mate_ref))
                ]

            for i in range(slots):
                for copy in copies(i, i):
                    copy.start()

            def step(i, carry):
                slot = lax.rem(i, slots)
                for s, copy in enumerate(copies(i, slot)):
                    copy.wait()
                    side = core if s == 0 else 1 - core
                    for b in range(top):
                        at = (side * top + b) ^ g
                        values = buffer[slot, s, b * span : (b + 1) * span, :]
                        first = values.astype(jnp.bfloat16)
                        large[i, at] = first
                        small[i, at] = (values - first.astype(jnp.float32)).astype(jnp.bfloat16)

                @pl.when(i + slots < count)
                def _():
                    for copy in copies(i + slots, slot):
                        copy.start()

                return carry

            lax.fori_loop(0, count, step, 0)

        shape = jax.ShapeDtypeStruct((count, groups, span, span), jnp.bfloat16)
        found = pl.pallas_call(
            kernel,
            out_shape=[shape] * 2,
            in_specs=[HBM] * 2,
            out_specs=[VMEM] * 2,
            scratch_shapes=[
                pltpu.VMEM((slots, 2, rows, span), jnp.float32),
                pltpu.SemaphoreType.DMA((slots, 2)),
            ],
            cost_estimate=pl.CostEstimate(
                flops=count << 24, bytes_accessed=count << 21, transcendentals=0
            ),
            compiler_params=pltpu.CompilerParams(vmem_limit_bytes=limit << 20),
        )(own.reshape(-1, rows, span), mates.reshape(-1, rows, span))
        return [values.reshape(end - begin, per, groups * span, span) for values in found]

    def rows_of(items):
        flat = [array for item in items for array in item]
        per, half = flat[0].shape[-3:-1]
        width = items[0][0].shape[-1] * len(items[0])
        counts = [item[0].shape[0] if item[0].ndim == 4 else 1 for item in items]
        total = sum(counts)

        def kernel(*refs):
            own_out, mate_out = refs[-2:]
            at, level_at = 0, 0
            for item, count in zip(items, counts, strict=True):
                mine = refs[at : at + len(item)]
                at += len(item)
                for n in range(count):
                    for k in range(per):
                        values = [ref[n, k] if ref.ndim == 4 else ref[k] for ref in mine]
                        if len(values) == 1:
                            values = split(values[0], groups)
                        own, mates = from_pieces(values)
                        own_out[level_at, k] = own
                        mate_out[level_at, k] = mates
                    level_at += 1

        return call(kernel, [(total, per, half, width // 2)] * 2, flat, 1000)

    def assemble(owns, theirs):
        per, half, span = owns[0].shape[-3:]
        total = sum(array.shape[0] for array in owns)

        def kernel(*refs):
            out = refs[-1]
            core, _ = place()
            for side, mine in ((core, refs[: len(owns)]), (1 - core, refs[len(owns) : -1])):
                rows = pl.ds(pl.multiple_of(side * half, half), half)
                at = 0
                for ref in mine:
                    for n in range(ref.shape[0]):
                        for k in range(per):
                            out[at, k, rows, :] = ref[n, k]
                        at += 1

        return call(kernel, [(total, per, 2 * half, span)], [*owns, *theirs], 1000)[0]

    def per_device(right_side, panels, diag_inverse, parents, live_width, tile_pattern):
        levels, per_level, rhs_count, row_span = right_side.shape
        col_span = panels.shape[3]
        half = rhs_count // 2
        piece = (per_level, half, col_span)
        work = 24 * per_level * half * row_span * col_span

        wide = (per_level, half, 2 * row_span)
        pair_list = [(h, g) for h in range(levels) for g in range(h + 1, levels)]

        def setup(parents_ref, width_ref, tiles_ref, col_out, row_out, weight_out):
            _, g = place()
            y_at, col_at = lax.axis_index("row") // 2, lax.axis_index("col")
            cells = lax.broadcasted_iota(jnp.int32, (1, col_span), 1)
            for h in range(levels):
                for k in range(per_level):
                    left = width_ref[h, k] - col_at * col_span
                    col_out[h, k] = jnp.where(cells < left, 1.0, 0.0)
                    for i in range(groups):
                        left = width_ref[h, k] - y_at * 2 * row_span - (g ^ i) * col_span
                        at = pl.ds(i * col_span, col_span)
                        row_out[h, k, :, at] = jnp.where(cells < left, 1.0, 0.0)
            per_group = col_span // TILE
            for slot, (low, high) in enumerate(pair_list):
                for k in range(per_level):
                    above = parents_ref[low, k]
                    for step in range(low + 1, high):
                        above = parents_ref[step, above]
                    for i in range(groups):
                        first = (y_at * groups + (g ^ i)) * per_group
                        for n in range(per_group):
                            present = tiles_ref[slot, k, first + n]
                            at = pl.ds(i * col_span + n * TILE, TILE)
                            for t in range(per_level):
                                kept = jnp.where(above == t, present, 0)
                                value = jnp.full((1, TILE), kept, jnp.int32)
                                weight_out[slot, k, t, :, at] = value.astype(jnp.float32)

        col_live, row_live, weight = call(
            setup,
            [
                (levels, per_level, 1, col_span),
                (levels, per_level, 1, 2 * row_span),
                (len(pair_list), per_level, per_level, 1, 2 * row_span),
            ],
            [parents, live_width, tile_pattern],
            1000,
            SMEM,
        )

        def down_diag(height, turned):
            at = 0 if height == 0 else height - 1

            def kernel(*refs):
                turned_refs, (mask, large, small), out = (
                    refs[:y_count],
                    refs[y_count : y_count + 3],
                    refs[y_count + 3 :],
                )
                for k in range(per_level):
                    x = sum(ref[k] for ref in turned_refs[1:]) + turned_refs[0][k]
                    x = x * mask[height, k]
                    pieces = split(product(x, large[at, k], small[at, k], 1), groups)
                    for i in range(groups):
                        out[i][k] = pieces[i]

            return call(kernel, [piece] * groups, [*turned, col_live, *diag_of(height)], work)

        def down_panel(height, turned, rest):
            slot = pair_index(height, height + 1, levels)
            at = slot if slot == 0 else slot - 1 if slot < levels else slot - levels

            def kernel(*refs):
                turned_refs = refs[:y_count]
                mask, weights, rest_ref, large, small = refs[y_count : y_count + 5]
                solved, out = refs[y_count + 5], refs[y_count + 6 :]
                left = [rest_ref[t] for t in range(per_level)]
                for k in range(per_level):
                    x = sum(ref[k] for ref in turned_refs[1:]) + turned_refs[0][k]
                    x = x * mask[height, k]
                    solved[k] = x
                    term = product(x, large[at, k], small[at, k], 1)
                    for t in range(per_level):
                        left[t] = left[t] - term * weights[slot, k, t]
                for t in range(per_level):
                    pieces = split(left[t], groups)
                    for i in range(groups):
                        out[i][t] = pieces[i]

            found = call(
                kernel,
                [piece] * (groups + 1),
                [*turned, col_live, weight, rest, *blocks_of(slot)],
                work,
            )
            return found[0], found[1:]

        def down_rest(height, higher, solved, rest):
            slot = pair_index(height, higher, levels)
            at = slot if slot == 0 else slot - 1 if slot < levels else slot - levels

            def kernel(x_ref, weights, rest_ref, large, small, out):
                left = [rest_ref[t] for t in range(per_level)]
                for k in range(per_level):
                    term = product(x_ref[k], large[at, k], small[at, k], 1)
                    for t in range(per_level):
                        left[t] = left[t] - term * weights[slot, k, t]
                for t in range(per_level):
                    out[t] = left[t]

            return call(kernel, [wide], [solved, weight, rest, *blocks_of(slot)], work)[0]

        def up_diag(height, received):
            at = 0 if height == 0 else height - 1

            def kernel(*refs):
                got = refs[:groups][::-1]
                mask, row_mask, large, small, out = refs[groups:]
                for k in range(per_level):
                    values = jnp.concatenate([ref[k] for ref in got], axis=-1)
                    values = values * row_mask[height, k]
                    out[k] = product(values, large[at, k], small[at, k], 0) * mask[height, k]

            return call(
                kernel, [piece], [*received[::-1], col_live, row_live, *diag_of(height)], work
            )[0]

        def only_first_y(values, fresh):
            if not fresh:
                return values
            return jnp.where(lax.axis_index("row") // 2 == 0, values, jnp.zeros_like(values))

        def up_panel(height, received, rest, fresh):
            slot = pair_index(height, height + 1, levels)
            at = slot if slot == 0 else slot - 1 if slot < levels else slot - levels

            def kernel(*refs):
                got = refs[:groups][::-1]
                weights, rest_ref, large, small, out, found = refs[groups:]
                values = []
                for t in range(per_level):
                    values.append(jnp.concatenate([ref[t] for ref in got], axis=-1))
                    found[t] = values[t]
                for k in range(per_level):
                    part = sum(values[t] * weights[slot, k, t] for t in range(per_level))
                    out[k] = only_first_y(rest_ref[k], fresh) - product(part, large[at, k], small[at, k], 0)

            return call(
                kernel, [piece, wide], [*received[::-1], weight, rest, *blocks_of(slot)], work
            )

        def up_rest(height, higher, found, rest, fresh):
            slot = pair_index(height, higher, levels)
            at = slot if slot == 0 else slot - 1 if slot < levels else slot - levels

            def kernel(found_ref, weights, rest_ref, large, small, out):
                for k in range(per_level):
                    part = sum(found_ref[t] * weights[slot, k, t] for t in range(per_level))
                    out[k] = only_first_y(rest_ref[k], fresh) - product(part, large[at, k], small[at, k], 0)

            return call(kernel, [piece], [found, weight, rest, *blocks_of(slot)], work)[0]

        def exchange(pieces):
            moved = [move(pieces[k], group_pairs[k]) for k in range(1, groups)]
            return sum(moved, pieces[0])

        def rows_to_cols(pieces):
            summed = exchange(pieces)
            return [move(summed, some) for some in turn_pairs[::-1]]

        def spread(block):
            return [block] + [move(block, group_pairs[k]) for k in range(1, groups)]

        def cols_to_rows(values):
            turned = [move(values, some) for some in back_pairs[::-1]]
            return spread(sum(turned[1:], turned[0]))

        def swap(values):
            return move(values, swap_pairs)

        def opening(side_ref, own_first, mate_first, own_rest, mate_rest):
            mine = place()[0]
            for which, first, others in ((mine, own_first, own_rest), (1 - mine, mate_first, mate_rest)):
                rows = pl.ds(pl.multiple_of(which * half, half), half)
                for k in range(per_level):
                    first[k] = side_ref[0, k, rows, :]
                    for h in range(1, levels):
                        others[h - 1, k] = side_ref[h, k, rows, :]

        one, rest_shape = (per_level, half, row_span), (levels - 1, per_level, half, row_span)
        own_first, give_first, own_others, give_others = call(
            opening, [one, one, rest_shape, rest_shape], [right_side], 1000
        )

        def first_piece(own_ref, mate_ref, out):
            for k in range(per_level):
                out[k] = to_pieces(own_ref[k], mate_ref[k])[0]

        def side_pieces(own_ref, mate_ref, *out):
            for h in range(levels - 1):
                for k in range(per_level):
                    values = jnp.concatenate(to_pieces(own_ref[h, k], mate_ref[h, k]), axis=-1)
                    out[h][k] = jnp.where(lax.axis_index("col") == 0, values, jnp.zeros_like(values))

        def take(diag_ref, block_ref, diag_out, block_out, done):
            copies = [
                pltpu.make_async_copy(ref.at[pl.ds(0, 1)], out, done.at[n])
                for n, (ref, out) in enumerate(((diag_ref, diag_out), (block_ref, block_out)))
            ]
            for copy in copies:
                copy.start()
            for copy in copies:
                copy.wait()

        mate_first = swap(give_first)
        head = jax.ShapeDtypeStruct((1, *diag_inverse.shape[1:]), jnp.float32)
        taken = pl.pallas_call(
            take,
            out_shape=[head] * 2,
            in_specs=[HBM] * 2,
            out_specs=[VMEM] * 2,
            scratch_shapes=[pltpu.SemaphoreType.DMA((2,))],
            name="take",
            cost_estimate=pl.CostEstimate(flops=1000, bytes_accessed=1 << 21, transcendentals=0),
            compiler_params=pltpu.CompilerParams(vmem_limit_bytes=60 << 20),
        )
        own_diag_first, own_block_first = taken(diag_inverse, panels)
        start = call(first_piece, [piece], [own_first, mate_first], 1000)[0]
        start = move(start, turn_pairs[0])
        mate_diag_first, mate_block_first = swap(own_diag_first), swap(own_block_first)
        mate_others = swap(give_others)
        diag_first = limbs(own_diag_first, mate_diag_first, 0, 1)
        blocks_first = limbs(own_block_first, mate_block_first, 0, 1)
        diag_first, blocks_first, diag_all, panels_all, col_live, row_live, weight = (
            lax.optimization_barrier(
                (
                    diag_first,
                    blocks_first,
                    diag_inverse,
                    panels,
                    col_live,
                    row_live,
                    weight,
                )
            )
        )
        mate_diag = swap(diag_all)
        mate_panels = swap(panels_all)
        diag_rest = limbs(diag_inverse, mate_diag, 1, levels, 8)
        blocks_near = limbs(panels, mate_panels, 1, levels, 42)
        blocks_rest = limbs(panels, mate_panels, levels, len(pair_list), 8)

        def diag_of(height):
            return diag_first if height == 0 else diag_rest

        def blocks_of(slot):
            return blocks_first if slot == 0 else blocks_near if slot < levels else blocks_rest

        rest = [None, *call(side_pieces, [wide] * (levels - 1), [own_others, mate_others], 1000)]
        turned = [start] + [jnp.zeros_like(start)] * (y_count - 1)
        interim = []
        for height in range(levels - 1):
            turned = rows_to_cols(down_diag(height, turned))
            solved, pieces = down_panel(height, turned, rest[height + 1])
            turned = rows_to_cols(pieces)
            for higher in range(height + 2, levels):
                rest[higher] = down_rest(height, higher, solved, rest[higher])
            interim.append(solved)

        pieces = down_diag(levels - 1, turned)
        summed = exchange(pieces)
        crossed = [move(summed, some) for some in cross_pairs]
        top_rows = received = spread(sum(crossed, summed))

        found = [None] * levels
        rest = list(interim)
        for height in reversed(range(levels)):
            received = cols_to_rows(up_diag(height, received))
            if height > 0:
                fresh = height == levels - 1
                sent, found[height] = up_panel(height - 1, received, rest[height - 1], fresh)
                received = cols_to_rows(sent)
                for lower in range(height - 1):
                    rest[lower] = up_rest(lower, height, found[height], rest[lower], fresh)

        def top_mask(*refs):
            got, mask, out = refs[:groups][::-1], refs[groups], refs[groups + 1]
            for k in range(per_level):
                values = jnp.concatenate([ref[k] for ref in got], axis=-1)
                out[k] = values * mask[levels - 1, k]

        lower_rows = spread(move(jnp.stack(interim), back_pairs[0]))
        top_wide = call(top_mask, [wide], [*top_rows[::-1], row_live], 1000)
        own, mates = rows_of([lower_rows, top_wide])
        interim_rows = assemble([own], [swap(mates)])

        own_higher, mate_higher = rows_of([[values] for values in found[1:]])
        theirs_higher = swap(mate_higher)
        own_lowest, mate_lowest = rows_of([received])
        solution_rows = assemble([own_lowest, own_higher], [swap(mate_lowest), theirs_higher])
        return interim_rows, solution_rows

    return jax.shard_map(
        per_device,
        mesh=mesh,
        in_specs=(
            P(None, None, None, "row"),
            P(None, None, "row", "col"),
            P(None, None, "row", "col"),
            P(),
            P(),
            P(),
        ),
        out_specs=(P(None, None, None, "row"), P(None, None, None, "row")),
        check_vma=False,
    )
```

```python
import jax
import jax.numpy as jnp
from jax import lax
from jax.experimental import pallas as pl
from jax.experimental.pallas import tpu as pltpu
from jax.sharding import PartitionSpec as P


TILE = 128


VMEM = pl.BlockSpec(memory_space=pltpu.VMEM)
SMEM = pl.BlockSpec(memory_space=pltpu.SMEM)
HBM = pl.BlockSpec(memory_space=pltpu.HBM)


def pair_index(lower, higher, depth_count):
    return lower * depth_count - lower * (lower + 1) // 2 + (higher - lower - 1)


def limbs_of(values, count):
    parts = []
    rest = values
    for i in range(count):
        part = rest.astype(jnp.bfloat16)
        parts.append(part)
        if i + 1 < count:
            rest = rest - part.astype(jnp.float32)
    return parts


def product(values, large, small, contract_block):
    m = values.shape[0]
    left = limbs_of(values, 3)
    total = None
    for block, count in ((small, 2), (large, 3)):
        found = lax.dot_general(
            jnp.concatenate(left[:count], axis=0),
            block,
            (((1,), (contract_block,)), ((), ())),
            preferred_element_type=jnp.float32,
        )
        for n in reversed(range(count)):
            part = found[n * m : (n + 1) * m]
            total = part if total is None else total + part
    return total


def solution(mesh):
    row_count, col_count = mesh.shape["row"], mesh.shape["col"]
    y_count = row_count // 2
    groups = col_count // y_count
    assert row_count == 2 * y_count and col_count == groups * y_count
    assert groups >= 2 and groups & (groups - 1) == 0
    top = groups // 2
    axes = ("row", "col")

    def pairs(move):
        found = []
        for row in range(row_count):
            for col in range(col_count):
                y, core, q, g = move(row // 2, row % 2, col // groups, col % groups)
                found.append((row * col_count + col, (2 * y + core) * col_count + groups * q + g))
        return found

    swap_pairs = pairs(lambda y, core, q, g: (y, 1 - core, q, g))
    group_pairs = [pairs(lambda y, core, q, g, k=k: (y, core, q, g ^ k)) for k in range(groups)]
    turn_pairs = [
        pairs(lambda y, core, q, g, t=t: ((q + t) % y_count, core, y, g)) for t in range(y_count)
    ]
    cross_pairs = [
        pairs(lambda y, core, q, g, t=t: (y, core, (q + t) % y_count, g))
        for t in range(1, y_count)
    ]
    back_pairs = [[(b, a) for a, b in some] for some in turn_pairs]

    def move(values, some):
        return lax.ppermute(values, axes, some)

    def place():
        row, col = lax.axis_index("row"), lax.axis_index("col")
        return row % 2, col % groups

    def reorder(pieces):
        _, g = place()
        bit = 1
        while bit < groups:
            on = (g & bit) != 0
            pieces = [jnp.where(on, pieces[k ^ bit], pieces[k]) for k in range(groups)]
            bit *= 2
        return pieces

    def split(values, count):
        span = values.shape[-1] // count
        return [values[..., i * span : (i + 1) * span] for i in range(count)]

    def to_pieces(own, mates):
        core, _ = place()
        first, second = jnp.where(core == 0, own, mates), jnp.where(core == 0, mates, own)
        return reorder(split(first, top) + split(second, top))

    def from_pieces(pieces):
        core, _ = place()
        pieces = reorder(pieces)
        first = jnp.concatenate(pieces[:top], axis=-1)
        second = jnp.concatenate(pieces[top:], axis=-1)
        return jnp.where(core == 0, first, second), jnp.where(core == 0, second, first)

    def call(kernel, outs, args, flops, space=VMEM):
        shapes = [jax.ShapeDtypeStruct(s, jnp.float32) for s in outs]
        return pl.pallas_call(
            kernel,
            out_shape=shapes,
            in_specs=[space] * len(args),
            out_specs=[VMEM] * len(outs),
            cost_estimate=pl.CostEstimate(flops=flops, bytes_accessed=1 << 20, transcendentals=0),
            compiler_params=pltpu.CompilerParams(vmem_limit_bytes=8 << 20),
        )(*args)

    def limbs(own, mates, begin, end, limit=8):
        rows, span = own.shape[-2:]
        per = own.shape[1]
        count = (end - begin) * per
        slots = min(4, count)

        def kernel(own_ref, mate_ref, large, small, buffer, done):
            core, g = place()

            def copies(i, slot):
                return [
                    pltpu.make_async_copy(ref.at[begin * per + i], buffer.at[slot, s], done.at[slot, s])
                    for s, ref in enumerate((own_ref, mate_ref))
                ]

            for i in range(slots):
                for copy in copies(i, i):
                    copy.start()

            def step(i, carry):
                slot = lax.rem(i, slots)
                for s, copy in enumerate(copies(i, slot)):
                    copy.wait()
                    side = core if s == 0 else 1 - core
                    for b in range(top):
                        at = (side * top + b) ^ g
                        values = buffer[slot, s, b * span : (b + 1) * span, :]
                        first = values.astype(jnp.bfloat16)
                        large[i, at] = first
                        small[i, at] = (values - first.astype(jnp.float32)).astype(jnp.bfloat16)

                @pl.when(i + slots < count)
                def _():
                    for copy in copies(i + slots, slot):
                        copy.start()

                return carry

            lax.fori_loop(0, count, step, 0)

        shape = jax.ShapeDtypeStruct((count, groups, span, span), jnp.bfloat16)
        found = pl.pallas_call(
            kernel,
            out_shape=[shape] * 2,
            in_specs=[HBM] * 2,
            out_specs=[VMEM] * 2,
            scratch_shapes=[
                pltpu.VMEM((slots, 2, rows, span), jnp.float32),
                pltpu.SemaphoreType.DMA((slots, 2)),
            ],
            cost_estimate=pl.CostEstimate(
                flops=count << 24, bytes_accessed=count << 21, transcendentals=0
            ),
            compiler_params=pltpu.CompilerParams(vmem_limit_bytes=limit << 20),
        )(own.reshape(-1, rows, span), mates.reshape(-1, rows, span))
        return [values.reshape(end - begin, per, groups * span, span) for values in found]

    def rows_of(items):
        flat = [array for item in items for array in item[::-1]]
        per, half = flat[0].shape[-3:-1]
        width = items[0][0].shape[-1] * len(items[0])
        counts = [item[0].shape[0] if item[0].ndim == 4 else 1 for item in items]
        total = sum(counts)

        def kernel(*refs):
            own_out, mate_out = refs[-2:]
            at, level_at = 0, 0
            for item, count in zip(items, counts, strict=True):
                mine = refs[at : at + len(item)][::-1]
                at += len(item)
                for n in range(count):
                    for k in range(per):
                        values = [ref[n, k] if ref.ndim == 4 else ref[k] for ref in mine]
                        if len(values) == 1:
                            values = split(values[0], groups)
                        own, mates = from_pieces(values)
                        own_out[level_at, k] = own
                        mate_out[level_at, k] = mates
                    level_at += 1

        return call(kernel, [(total, per, half, width // 2)] * 2, flat, 1000)

    def assemble(owns, theirs):
        per, half, span = owns[0].shape[-3:]
        total = sum(array.shape[0] for array in owns)

        def kernel(*refs):
            out = refs[-1]
            core, _ = place()
            for side, mine in ((core, refs[: len(owns)]), (1 - core, refs[len(owns) : -1])):
                rows = pl.ds(pl.multiple_of(side * half, half), half)
                at = 0
                for ref in mine:
                    for n in range(ref.shape[0]):
                        for k in range(per):
                            out[at, k, rows, :] = ref[n, k]
                        at += 1

        return call(kernel, [(total, per, 2 * half, span)], [*owns, *theirs], 1000)[0]

    def per_device(right_side, panels, diag_inverse, parents, live_width, tile_pattern):
        levels, per_level, rhs_count, row_span = right_side.shape
        col_span = panels.shape[3]
        half = rhs_count // 2
        piece = (per_level, half, col_span)
        work = 24 * per_level * half * row_span * col_span

        wide = (per_level, half, 2 * row_span)
        pair_list = [(h, g) for h in range(levels) for g in range(h + 1, levels)]

        def setup(parents_ref, width_ref, tiles_ref, col_out, row_out, weight_out):
            _, g = place()
            y_at, col_at = lax.axis_index("row") // 2, lax.axis_index("col")
            cells = lax.broadcasted_iota(jnp.int32, (1, col_span), 1)
            for h in range(levels):
                for k in range(per_level):
                    left = width_ref[h, k] - col_at * col_span
                    col_out[h, k] = jnp.where(cells < left, 1.0, 0.0)
                    for i in range(groups):
                        left = width_ref[h, k] - y_at * 2 * row_span - (g ^ i) * col_span
                        at = pl.ds(i * col_span, col_span)
                        row_out[h, k, :, at] = jnp.where(cells < left, 1.0, 0.0)
            per_group = col_span // TILE
            for slot, (low, high) in enumerate(pair_list):
                for k in range(per_level):
                    above = parents_ref[low, k]
                    for step in range(low + 1, high):
                        above = parents_ref[step, above]
                    for i in range(groups):
                        first = (y_at * groups + (g ^ i)) * per_group
                        for n in range(per_group):
                            present = tiles_ref[slot, k, first + n]
                            at = pl.ds(i * col_span + n * TILE, TILE)
                            for t in range(per_level):
                                kept = jnp.where(above == t, present, 0)
                                value = jnp.full((1, TILE), kept, jnp.int32)
                                weight_out[slot, k, t, :, at] = value.astype(jnp.float32)

        col_live, row_live, weight = call(
            setup,
            [
                (levels, per_level, 1, col_span),
                (levels, per_level, 1, 2 * row_span),
                (len(pair_list), per_level, per_level, 1, 2 * row_span),
            ],
            [parents, live_width, tile_pattern],
            1000,
            SMEM,
        )

        def down_diag(height, turned):
            at = 0 if height == 0 else height - 1

            def kernel(*refs):
                turned_refs, (mask, large, small), out = (
                    refs[:y_count],
                    refs[y_count : y_count + 3],
                    refs[y_count + 3 :],
                )
                for k in range(per_level):
                    x = sum(ref[k] for ref in turned_refs[1:]) + turned_refs[0][k]
                    x = x * mask[height, k]
                    pieces = split(product(x, large[at, k], small[at, k], 1), groups)
                    for i in range(groups):
                        out[i][k] = pieces[i]

            return call(kernel, [piece] * groups, [*turned, col_live, *diag_of(height)], work)

        def down_panel(height, turned, rest):
            slot = pair_index(height, height + 1, levels)
            at = slot if slot == 0 else slot - 1 if slot < levels else slot - levels

            def kernel(*refs):
                turned_refs = refs[:y_count]
                mask, weights, rest_ref, large, small = refs[y_count : y_count + 5]
                solved, out = refs[y_count + 5], refs[y_count + 6 :]
                left = [rest_ref[t] for t in range(per_level)]
                for k in range(per_level):
                    x = sum(ref[k] for ref in turned_refs[1:]) + turned_refs[0][k]
                    x = x * mask[height, k]
                    solved[k] = x
                    term = product(x, large[at, k], small[at, k], 1)
                    for t in range(per_level):
                        left[t] = left[t] - term * weights[slot, k, t]
                for t in range(per_level):
                    pieces = split(left[t], groups)
                    for i in range(groups):
                        out[i][t] = pieces[i]

            found = call(
                kernel,
                [piece] * (groups + 1),
                [*turned, col_live, weight, rest, *blocks_of(slot)],
                work,
            )
            return found[0], found[1:]

        def down_rest(height, higher, solved, rest):
            slot = pair_index(height, higher, levels)
            at = slot if slot == 0 else slot - 1 if slot < levels else slot - levels

            def kernel(x_ref, weights, rest_ref, large, small, out):
                left = [rest_ref[t] for t in range(per_level)]
                for k in range(per_level):
                    term = product(x_ref[k], large[at, k], small[at, k], 1)
                    for t in range(per_level):
                        left[t] = left[t] - term * weights[slot, k, t]
                for t in range(per_level):
                    out[t] = left[t]

            return call(kernel, [wide], [solved, weight, rest, *blocks_of(slot)], work)[0]

        def up_diag(height, received):
            at = 0 if height == 0 else height - 1

            def kernel(*refs):
                got = refs[:groups][::-1]
                mask, row_mask, large, small, out = refs[groups:]
                for k in range(per_level):
                    values = jnp.concatenate([ref[k] for ref in got], axis=-1)
                    values = values * row_mask[height, k]
                    out[k] = product(values, large[at, k], small[at, k], 0) * mask[height, k]

            return call(
                kernel, [piece], [*received[::-1], col_live, row_live, *diag_of(height)], work
            )[0]

        def only_first_y(values, fresh):
            if not fresh:
                return values
            return jnp.where(lax.axis_index("row") // 2 == 0, values, jnp.zeros_like(values))

        def up_panel(height, received, rest, fresh):
            slot = pair_index(height, height + 1, levels)
            at = slot if slot == 0 else slot - 1 if slot < levels else slot - levels

            def kernel(*refs):
                got = refs[:groups][::-1]
                weights, rest_ref, large, small, out, found = refs[groups:]
                values = []
                for t in range(per_level):
                    values.append(jnp.concatenate([ref[t] for ref in got], axis=-1))
                    found[t] = values[t]
                for k in range(per_level):
                    part = sum(values[t] * weights[slot, k, t] for t in range(per_level))
                    out[k] = only_first_y(rest_ref[k], fresh) - product(part, large[at, k], small[at, k], 0)

            return call(
                kernel, [piece, wide], [*received[::-1], weight, rest, *blocks_of(slot)], work
            )

        def up_rest(height, higher, found, rest, fresh):
            slot = pair_index(height, higher, levels)
            at = slot if slot == 0 else slot - 1 if slot < levels else slot - levels

            def kernel(found_ref, weights, rest_ref, large, small, out):
                for k in range(per_level):
                    part = sum(found_ref[t] * weights[slot, k, t] for t in range(per_level))
                    out[k] = only_first_y(rest_ref[k], fresh) - product(part, large[at, k], small[at, k], 0)

            return call(kernel, [piece], [found, weight, rest, *blocks_of(slot)], work)[0]

        def exchange(pieces):
            moved = [move(pieces[k], group_pairs[k]) for k in range(1, groups)]
            return sum(moved, pieces[0])

        def rows_to_cols(pieces):
            summed = exchange(pieces)
            return [move(summed, some) for some in turn_pairs[::-1]]

        def spread(block):
            return [block] + [move(block, group_pairs[k]) for k in range(1, groups)]

        def cols_to_rows(values):
            turned = [move(values, some) for some in back_pairs[::-1]]
            return spread(sum(turned[1:], turned[0]))

        def swap(values):
            return move(values, swap_pairs)

        def opening(side_ref, own_first, mate_first, own_rest, mate_rest):
            mine = place()[0]
            for which, first, others in ((mine, own_first, own_rest), (1 - mine, mate_first, mate_rest)):
                rows = pl.ds(pl.multiple_of(which * half, half), half)
                for k in range(per_level):
                    first[k] = side_ref[0, k, rows, :]
                    for h in range(1, levels):
                        others[h - 1, k] = side_ref[h, k, rows, :]

        one, rest_shape = (per_level, half, row_span), (levels - 1, per_level, half, row_span)
        own_first, give_first, own_others, give_others = call(
            opening, [one, one, rest_shape, rest_shape], [right_side], 1000
        )

        def first_piece(own_ref, mate_ref, out):
            for k in range(per_level):
                out[k] = to_pieces(own_ref[k], mate_ref[k])[0]

        def side_pieces(own_ref, mate_ref, *out):
            for h in range(levels - 1):
                for k in range(per_level):
                    values = jnp.concatenate(to_pieces(own_ref[h, k], mate_ref[h, k]), axis=-1)
                    out[h][k] = jnp.where(lax.axis_index("col") == 0, values, jnp.zeros_like(values))

        def take(diag_ref, block_ref, diag_out, block_out, done):
            copies = [
                pltpu.make_async_copy(ref.at[pl.ds(0, 1)], out, done.at[n])
                for n, (ref, out) in enumerate(((diag_ref, diag_out), (block_ref, block_out)))
            ]
            for copy in copies:
                copy.start()
            for copy in copies:
                copy.wait()

        mate_first = swap(give_first)
        head = jax.ShapeDtypeStruct((1, *diag_inverse.shape[1:]), jnp.float32)
        taken = pl.pallas_call(
            take,
            out_shape=[head] * 2,
            in_specs=[HBM] * 2,
            out_specs=[VMEM] * 2,
            scratch_shapes=[pltpu.SemaphoreType.DMA((2,))],
            name="take",
            cost_estimate=pl.CostEstimate(flops=1000, bytes_accessed=1 << 21, transcendentals=0),
            compiler_params=pltpu.CompilerParams(vmem_limit_bytes=60 << 20),
        )
        own_diag_first, own_block_first = taken(diag_inverse, panels)
        start = call(first_piece, [piece], [own_first, mate_first], 1000)[0]
        start = move(start, turn_pairs[0])
        mate_diag_first, mate_block_first = swap(own_diag_first), swap(own_block_first)
        mate_others = swap(give_others)
        diag_first = limbs(own_diag_first, mate_diag_first, 0, 1)
        blocks_first = limbs(own_block_first, mate_block_first, 0, 1)
        diag_first, blocks_first, diag_all, panels_all, col_live, row_live, weight = (
            lax.optimization_barrier(
                (
                    diag_first,
                    blocks_first,
                    diag_inverse,
                    panels,
                    col_live,
                    row_live,
                    weight,
                )
            )
        )
        mate_diag = swap(diag_all)
        mate_panels = swap(panels_all)
        diag_rest = limbs(diag_inverse, mate_diag, 1, levels, 8)
        blocks_near = limbs(panels, mate_panels, 1, levels, 8)
        blocks_rest = limbs(panels, mate_panels, levels, len(pair_list), 8)

        def diag_of(height):
            return diag_first if height == 0 else diag_rest

        def blocks_of(slot):
            return blocks_first if slot == 0 else blocks_near if slot < levels else blocks_rest

        rest = [None, *call(side_pieces, [wide] * (levels - 1), [own_others, mate_others], 1000)]
        turned = [start] + [jnp.zeros_like(start)] * (y_count - 1)
        interim = []
        for height in range(levels - 1):
            turned = rows_to_cols(down_diag(height, turned))
            solved, pieces = down_panel(height, turned, rest[height + 1])
            turned = rows_to_cols(pieces)
            for higher in range(height + 2, levels):
                rest[higher] = down_rest(height, higher, solved, rest[higher])
            interim.append(solved)

        pieces = down_diag(levels - 1, turned)
        summed = exchange(pieces)
        crossed = [move(summed, some) for some in cross_pairs]
        top_rows = received = spread(sum(crossed, summed))

        found = [None] * levels
        rest = list(interim)
        for height in reversed(range(levels)):
            received = cols_to_rows(up_diag(height, received))
            if height > 0:
                fresh = height == levels - 1
                sent, found[height] = up_panel(height - 1, received, rest[height - 1], fresh)
                received = cols_to_rows(sent)
                for lower in range(height - 1):
                    rest[lower] = up_rest(lower, height, found[height], rest[lower], fresh)

        def top_mask(*refs):
            got, mask, out = refs[:groups][::-1], refs[groups], refs[groups + 1]
            for k in range(per_level):
                values = jnp.concatenate([ref[k] for ref in got], axis=-1)
                out[k] = values * mask[levels - 1, k]

        lower_rows = spread(move(jnp.stack(interim), back_pairs[0]))
        top_wide = call(top_mask, [wide], [*top_rows[::-1], row_live], 1000)
        own, mates = rows_of([lower_rows, top_wide])
        interim_rows = assemble([own], [swap(mates)])

        own_higher, mate_higher = rows_of([[values] for values in found[1:]])
        theirs_higher = swap(mate_higher)
        own_lowest, mate_lowest = rows_of([received])
        solution_rows = assemble([own_lowest, own_higher], [swap(mate_lowest), theirs_higher])
        return interim_rows, solution_rows

    return jax.shard_map(
        per_device,
        mesh=mesh,
        in_specs=(
            P(None, None, None, "row"),
            P(None, None, "row", "col"),
            P(None, None, "row", "col"),
            P(),
            P(),
            P(),
        ),
        out_specs=(P(None, None, None, "row"), P(None, None, None, "row")),
        check_vma=False,
    )
```
